256 devices in a mesh: edge: 64 (over y, z, x_lo), chan: 4 (over x_hi, core).
Axes of the slice: x: 4 (x_hi: 2, x_lo: 2; x = x_hi * 2 + x_lo), y: 4, z: 8, core: 2. Of those that a mesh axis runs over, the one named last changes fastest.
Arguments:
- node_states: bfloat16 [1024, 49, 256], P('edge', None, 'chan'), may hold values from -6 to 6
- edge_vectors: float32 [3, 32768], P(None, ('edge', 'chan')), may hold values from -5.6 to 5.6, as said below
- source_part: int32 [32768, 1], P('edge'), may hold values from 0 to 63; in each aligned block of 512 rows (0 to 511, 512 to 1023, ...) at most 16 rows name the same one
- source_slot: int32 [32768], P('edge'), may hold values from 0 to 15
- target_slot: int32 [32768], P('edge'), may hold values from 0 to 15
- live_edges: int32 [64], P('edge'), may hold values from 1 to 512, 24576 in all
- weight_zero: bfloat16 [7, 256, 7, 256], P(None, 'chan'), may hold values from -0.125 to 0.125
- weight_one: bfloat16 [2, 6, 256, 6, 256], P(None, None, 'chan'), may hold values from -0.109375 to 0.109375
- weight_two: bfloat16 [2, 5, 256, 5, 256], P(None, None, 'chan'), may hold values from -0.125 to 0.125
Outputs:
- aggregated: bfloat16 [1024, 49, 256], P('edge', None, 'chan')
The draws below stay inside these ranges and needn't reach their ends.
Inputs may be any that keep to these rules, and one draw needn't show every extreme that they name: `source_part`: in each aligned block of 512 rows (the edges of one partition's slab) no partition number appears more than 16 times, and some number appears exactly 16 times. Edges are grouped by destination partition: the destination of an edge in slab p is node p * 16 + target_slot. `live_edges`: live slots stand at the front of each slab; the fullest slab is full. `edge_vectors`: every column has length between 0.8 and 5.6.
All inputs are finite; a program needn't handle non-finite values. No bound on the sum of `live_edges` on one device may be relied on, other than what follows from the above.
Results may differ from the reference program's by a relative error of at most 0.015.
Values may be sent and summed in bfloat16 or wider, within the bound.
A program may use at most 128 MiB of HBM per device.

```python
import math
import jax
import jax.numpy as jnp
import numpy as np
from jax import lax

C = 256
LMAX = 6
MMAX = 2
N_DEV = 16
E_CAP = 512
NODES = 1024
EDGES = 32768
CAP = 16
COEFS = 49
KEPT = 29
N_EDGE = 64
N_CHAN = 4


def draw_edge_vectors(key, part):
    first_key, second_key = jax.random.split(jax.random.fold_in(key, 17))
    raw = jax.random.normal(first_key, (3, EDGES), jnp.float32)
    length = jax.random.uniform(second_key, (1, EDGES), jnp.float32, 0.8, 5.6)
    norm_value = jnp.sqrt(jnp.sum(raw * raw, axis=0, keepdims=True))
    direction = raw / jnp.maximum(norm_value, 1e-06)
    return jnp.clip(direction * length, -5.6, 5.6)


def with_ends(entries, rng, smallest, largest):
    index_at = [jax.random.randint(jax.random.fold_in(rng, axis), (), 0, length) for axis, length in enumerate(entries.shape)]
    longest = entries.shape.index(max(entries.shape))
    beside = index_at[:longest] + [(index_at[longest] + 1) % entries.shape[longest]] + index_at[longest + 1:]
    return entries.at[tuple(index_at)].set(smallest).at[tuple(beside)].set(largest)


def level_of(stream_key, shape, cuts, smallest, high):
    gain = 1.0
    for dim, shards_of in cuts:
        draws = jax.random.uniform(jax.random.fold_in(jax.random.fold_in(stream_key, 6), dim), (shards_of,), jnp.float32, smallest / len(cuts), high / len(cuts))
        gain = gain * jnp.repeat(jnp.exp(draws), shape[dim] // shards_of).reshape((-1,) + (1,) * (len(shape) - 1 - dim))
    return gain


def length_profile(number_of, total, bound, skew):
    portions = [(1 << 20) // math.isqrt(rank ** skew) + 1 for rank in range(2, number_of + 1)]
    spare, given = total - bound - (number_of - 1), [1] * (number_of - 1)
    while spare > 0:
        movable = [i for i in range(number_of - 1) if given[i] < bound]
        mass, budget = sum([portions[i] for i in movable]), spare
        for i in movable:
            more = min(bound - given[i], max(1, budget * portions[i] // mass), spare)
            given[i] = given[i] + more
            spare = spare - more
    return np.array([bound] + given)


def uneven_parts(stream_key, count, total, limit, lean):
    if count == 2:
        one = jax.random.randint(stream_key, (), max(1, total - limit), min(limit, total - 1) + 1)
        return jnp.stack([one, total - one])
    lengths = jnp.asarray(length_profile(count, total, limit, lean), jnp.int32)
    twos = (count - 1) // 2
    source_of, receiver = lengths[1:1 + 2 * twos:2], lengths[2:2 + 2 * twos:2]
    slack = jnp.minimum(source_of - 1, limit - receiver)
    passed = jax.random.randint(jax.random.fold_in(stream_key, 1), (twos,), 0, 1 << 20) % (slack + 1)
    lengths = lengths.at[1:1 + 2 * twos:2].set(source_of - passed).at[2:2 + 2 * twos:2].set(receiver + passed)
    return lengths[jax.random.permutation(jax.random.fold_in(stream_key, 2), count)]


def assign_block(own_key, own, number, rows, amount, top, most, lean):
    sequence = jax.random.permutation(own_key, amount)
    packed, usual = load_shares(amount, rows * top, most, lean, True), load_shares(amount, rows * top, most, lean, False)
    places = jnp.arange(amount)

    def named(sizes, turn):
        used = int((sizes > 0).sum())
        fixed = max(1, used // 4)
        passed = fixed + (places - fixed + turn * (used - fixed)) % max(1, amount - fixed)
        return jnp.zeros((amount,), jnp.int32).at[sequence[jnp.where(places < fixed, places, passed)]].set(jnp.asarray(sizes, jnp.int32))

    sizes = jnp.where(number % 4 == 0, named(packed, number // 4), named(usual, number - number // 4 - 1))
    mixed = jax.random.permutation(jax.random.fold_in(own, 3), amount)
    giver, receiver = mixed[0:amount // 2 * 2:2], mixed[1:amount // 2 * 2:2]
    room = jnp.minimum(sizes[giver] - 1, most - sizes[receiver]) // 2
    room = jnp.where((giver == sequence[0]) | (receiver == sequence[0]) | (sizes[receiver] == 0), 0, jnp.maximum(room, 0))
    passed = jax.random.randint(jax.random.fold_in(own, 4), (amount // 2,), 0, 1 << 20) % (room + 1)
    sizes = sizes.at[giver].add(-passed).at[receiver].add(passed)
    labels = jnp.searchsorted(jnp.cumsum(sizes), jnp.arange(rows * top), side="right").astype(jnp.int32)
    table = labels.reshape(top, rows).T
    table = table[jax.random.permutation(jax.random.fold_in(own, 1), rows)]
    turn = jax.random.randint(jax.random.fold_in(own, 2), (rows, 1), 0, top)
    return jnp.take_along_axis(table, (jnp.arange(top)[None, :] + turn) % top, axis=1)


def load_shares(count, total, bound, lean, full):
    loads = [(1 << 20) // math.isqrt(grade ** lean) + 1 for grade in range(1, count + 1)]
    largest = bound if full else min(bound, max(-(-total // count), total * loads[0] // sum(loads)))
    least = 1 if total - largest >= count - 1 else 0
    counts, rest = [largest] + [least] * (count - 1), total - largest - least * (count - 1)
    while rest > 0:
        movable = [i for i in range(1, count) if counts[i] < largest] or [i for i in range(1, count) if counts[i] < bound]
        mass, budget = sum([loads[i] for i in movable]), rest
        for i in movable:
            addition = min(bound - counts[i], max(1, budget * loads[i] // mass), rest)
            counts[i] = counts[i] + addition
            rest = rest - addition
    return np.array(counts)


def scatter_about(stream_key, shape, width, bound, cuts=(), kind=jnp.bfloat16):
    result = width * jax.random.normal(stream_key, shape, jnp.float32)
    if cuts:
        result = result * level_of(stream_key, shape, cuts, -0.22, 0.18)
    return jnp.clip(result, -bound, bound).astype(kind)


def setup_inputs(seed: int = 0) -> dict:
    splits = jax.random.split(jax.random.key(seed), 10)
    node_states = scatter_about(splits[0], (NODES, COEFS, C), 1.0, 6.0, ((0, 64), (2, 4)))
    edge_vectors = draw_edge_vectors(jax.random.fold_in(splits[9], 71), 0)
    source_part_keys = jax.random.split(jax.random.fold_in(splits[2], 1), EDGES // E_CAP)
    source_part_turns = jax.random.permutation(jax.random.fold_in(splits[2], 3), EDGES // E_CAP)
    source_part = jax.vmap(lambda own, number: assign_block(jax.random.fold_in(splits[2], 2), own, number, E_CAP, N_EDGE, 1, CAP, 2))(source_part_keys, source_part_turns).reshape((EDGES, 1))
    source_slot = with_ends(jax.random.randint(splits[3], (EDGES,), 0, N_DEV), jax.random.fold_in(splits[3], 1), 0, N_DEV - 1).astype(jnp.int32)
    target_slot = with_ends(jax.random.randint(splits[4], (EDGES,), 0, N_DEV), jax.random.fold_in(splits[4], 1), 0, N_DEV - 1).astype(jnp.int32)
    live_edges = uneven_parts(splits[5], N_EDGE, (3 * E_CAP * N_EDGE) // 4, E_CAP, 2).astype(jnp.int32)
    weight_zero = scatter_about(splits[6], (LMAX + 1, C, LMAX + 1, C), ((LMAX + 1) * C) ** -0.5, 0.125, ((1, 4),))
    weight_one = scatter_about(splits[7], (2, LMAX, C, LMAX, C), (2 * LMAX * C) ** -0.5, 0.109375, ((2, 4),))
    weight_two = scatter_about(splits[8], (2, LMAX - 1, C, LMAX - 1, C), (2 * (LMAX - 1) * C) ** -0.5, 0.125, ((2, 4),))
    return {"node_states": node_states, "edge_vectors": edge_vectors, "source_part": source_part, "source_slot": source_slot, "target_slot": target_slot, "live_edges": live_edges, "weight_zero": weight_zero, "weight_one": weight_one, "weight_two": weight_two}


cutoff_radius = 6.0
highest = lax.Precision.HIGHEST

def harmonics(coord_x, coord_y, coord_z, degree_top, order_top):
    results = {}
    real_part = [coord_x * 0.0 + 1.0]
    imag_part = [coord_x * 0.0]
    for azimuthal in range(1, order_top + 1):
        new_real = coord_x * real_part[-1] - coord_y * imag_part[-1]
        new_imag = coord_x * imag_part[-1] + coord_y * real_part[-1]
        real_part.append(new_real)
        imag_part.append(new_imag)
    for azimuthal in range(order_top + 1):
        start_value = (-1.0) ** azimuthal * math.prod(range(2 * azimuthal - 1, 0, -2))
        legendre = {azimuthal: coord_z * 0.0 + start_value}
        if azimuthal + 1 <= degree_top:
            legendre[azimuthal + 1] = coord_z * ((2 * azimuthal + 1) * start_value)
        for degree in range(azimuthal + 2, degree_top + 1):
            legendre[degree] = ((2 * degree - 1) * coord_z * legendre[degree - 1] - (degree + azimuthal - 1) * legendre[degree - 2]) / (degree - azimuthal)
        for degree in range(azimuthal, degree_top + 1):
            factor = math.sqrt((2 * degree + 1) / (4.0 * math.pi) * math.factorial(degree - azimuthal) / math.factorial(degree + azimuthal))
            if azimuthal == 0:
                results[degree, 0] = factor * legendre[degree]
            else:
                results[degree, azimuthal] = math.sqrt(2.0) * factor * legendre[degree] * real_part[azimuthal]
                results[degree, -azimuthal] = math.sqrt(2.0) * factor * legendre[degree] * imag_part[azimuthal]
    return results

def kept_rows():
    row_list = [(degree, 0) for degree in range(LMAX + 1)]
    for azimuthal in range(1, MMAX + 1):
        row_list += [(degree, azimuthal) for degree in range(azimuthal, LMAX + 1)]
        row_list += [(degree, -azimuthal) for degree in range(azimuthal, LMAX + 1)]
    return row_list

def invert_small(matrix):
    order_size = matrix.shape[0]
    work = np.concatenate([matrix, np.eye(order_size)], axis=1)
    for column in range(order_size):
        work[column] = work[column] / work[column, column]
        for row_index in range(order_size):
            if row_index != column:
                work[row_index] = work[row_index] - work[row_index, column] * work[column]
    return work[:, order_size:]

def sample_tables():
    sample_count = 2 * (LMAX + 1) ** 2
    positions = np.arange(sample_count) + 0.5
    height = 1.0 - 2.0 * positions / sample_count
    radius = np.sqrt(1.0 - height * height)
    azimuth = math.pi * (3.0 - math.sqrt(5.0)) * positions
    points = np.stack([radius * np.cos(azimuth), radius * np.sin(azimuth), height])
    values = harmonics(points[0], points[1], points[2], LMAX, LMAX)
    inverses = []
    for degree in range(LMAX + 1):
        sampled = np.stack([values[degree, azimuthal] for azimuthal in range(-degree, degree + 1)])
        inverses.append(sampled.T @ invert_small(sampled @ sampled.T))
    return (points, inverses)

def wigner_rows(vectors):
    length = jnp.sqrt(lax.optimization_barrier(jnp.sum(vectors * vectors, axis=0)))
    direction = vectors / length
    pick_first = jnp.where(jnp.abs(direction[0]) < 0.6, 1.0, 0.0).astype(jnp.float32)
    helper = jnp.stack([pick_first, 1.0 - pick_first, jnp.zeros_like(pick_first)])
    first_axis = jnp.cross(direction, helper, axis=0)
    first_axis = first_axis / jnp.sqrt(lax.optimization_barrier(jnp.sum(first_axis * first_axis, axis=0)))
    second_axis = jnp.cross(direction, first_axis, axis=0)
    frames = jnp.stack([first_axis, second_axis, direction])
    points, inverses = sample_tables()
    sample = jnp.asarray(points, jnp.float32)
    turned = jnp.einsum('rce,ck->rek', frames, sample, precision=highest)
    values = harmonics(turned[0], turned[1], turned[2], LMAX, MMAX)
    pieces = []
    for degree, azimuthal in kept_rows():
        table = jnp.asarray(inverses[degree], jnp.float32)
        pieces.append(jnp.dot(values[degree, azimuthal], table, precision=highest))
    compact = jnp.concatenate(pieces, axis=1)
    envelope = 0.5 * (jnp.cos(math.pi * length / cutoff_radius) + 1.0)
    return (compact, envelope)

def expand_rows(compact):
    padded_rows = []
    offset = 0
    for degree, azimuthal in kept_rows():
        span_size = 2 * degree + 1
        segment = compact[:, offset:offset + span_size]
        padded_rows.append(jnp.pad(segment, ((0, 0), (degree * degree, (LMAX + 1) ** 2 - degree * degree - span_size))))
        offset += span_size
    return jnp.stack(padded_rows, axis=1)

def convolve(turned, weight_zero, weight_one, weight_two, contract):
    end_zero = LMAX + 1
    end_one_plus = end_zero + LMAX
    end_one_minus = end_one_plus + LMAX
    end_two_plus = end_one_minus + LMAX - 1
    zero_part = turned[:end_zero]
    one_plus = turned[end_zero:end_one_plus]
    one_minus = turned[end_one_plus:end_one_minus]
    two_plus = turned[end_one_minus:end_two_plus]
    two_minus = turned[end_two_plus:]
    pattern = 'lce,lcjd->dje'
    out_zero = contract(pattern, zero_part, weight_zero)
    out_one_plus = contract(pattern, one_plus, weight_one[0]) - contract(pattern, one_minus, weight_one[1])
    out_one_minus = contract(pattern, one_minus, weight_one[0]) + contract(pattern, one_plus, weight_one[1])
    out_two_plus = contract(pattern, two_plus, weight_two[0]) - contract(pattern, two_minus, weight_two[1])
    out_two_minus = contract(pattern, two_minus, weight_two[0]) + contract(pattern, two_plus, weight_two[1])
    return jnp.concatenate([out_zero, out_one_plus, out_one_minus, out_two_plus, out_two_minus], axis=1)

def rounded(values):
    return lax.optimization_barrier(values.astype(jnp.bfloat16))

def float_contract(pattern, first_operand, second_operand):
    return jnp.einsum(pattern, first_operand.astype(jnp.float32), second_operand.astype(jnp.float32))

def reference(node_states, edge_vectors, source_part, source_slot, target_slot, live_edges, weight_zero, weight_one, weight_two):
    per_group = C // N_CHAN

    def one_slab(partition):
        first_edge = (partition * E_CAP).astype(jnp.int32)
        vectors = lax.dynamic_slice_in_dim(edge_vectors, first_edge, E_CAP, 1)
        compact, envelope = wigner_rows(vectors)
        rotation = expand_rows(rounded(compact))
        owner_part = lax.dynamic_slice_in_dim(source_part[:, 0], first_edge, E_CAP, 0)
        source_slots = lax.dynamic_slice_in_dim(source_slot, first_edge, E_CAP, 0)
        targets = lax.dynamic_slice_in_dim(target_slot, first_edge, E_CAP, 0)
        sources = node_states[owner_part * N_DEV + source_slots]
        turned = rounded(jnp.einsum('eik,ekc->ice', rotation.astype(jnp.float32), sources.astype(jnp.float32)))
        channel_mix = jnp.zeros((C, KEPT, E_CAP), jnp.float32)
        for group_index in range(N_CHAN):
            low_channel = group_index * per_group
            high_channel = low_channel + per_group
            partial_value = convolve(turned[:, low_channel:high_channel], weight_zero[:, low_channel:high_channel], weight_one[:, :, low_channel:high_channel], weight_two[:, :, low_channel:high_channel], float_contract)
            channel_mix = channel_mix + rounded(partial_value).astype(jnp.float32)
        alive_mask = (jnp.arange(E_CAP, dtype=jnp.int32) < live_edges[partition]).astype(jnp.float32)
        scaling = rounded(envelope).astype(jnp.float32) * alive_mask
        scaled = rounded(channel_mix * scaling)
        message = rounded(jnp.einsum('eik,cie->ekc', rotation.astype(jnp.float32), scaled.astype(jnp.float32)))
        selector = (jnp.arange(N_DEV, dtype=jnp.int32)[:, None] == targets[None, :]).astype(jnp.bfloat16)
        summed = jnp.dot(selector, message.reshape(E_CAP, COEFS * C), preferred_element_type=jnp.float32)
        return summed.astype(jnp.bfloat16).reshape(N_DEV, COEFS, C)
    blocks = lax.map(one_slab, jnp.arange(N_EDGE, dtype=jnp.int32))
    return blocks.reshape(NODES, COEFS, C)
```

```python
import math

import jax
import jax.numpy as jnp
import numpy as np
from jax import lax
from jax.sharding import PartitionSpec as P

LMAX = 6
MMAX = 2


cutoff_radius = 6.0
highest = lax.Precision.HIGHEST


def harmonics(coord_x, coord_y, coord_z, degree_top, order_top):
    results = {}
    real_part = [coord_x * 0.0 + 1.0]
    imag_part = [coord_x * 0.0]
    for azimuthal in range(1, order_top + 1):
        new_real = coord_x * real_part[-1] - coord_y * imag_part[-1]
        new_imag = coord_x * imag_part[-1] + coord_y * real_part[-1]
        real_part.append(new_real)
        imag_part.append(new_imag)
    for azimuthal in range(order_top + 1):
        start_value = (-1.0) ** azimuthal * math.prod(range(2 * azimuthal - 1, 0, -2))
        legendre = {azimuthal: coord_z * 0.0 + start_value}
        if azimuthal + 1 <= degree_top:
            legendre[azimuthal + 1] = coord_z * ((2 * azimuthal + 1) * start_value)
        for degree in range(azimuthal + 2, degree_top + 1):
            legendre[degree] = (
                (2 * degree - 1) * coord_z * legendre[degree - 1]
                - (degree + azimuthal - 1) * legendre[degree - 2]
            ) / (degree - azimuthal)
        for degree in range(azimuthal, degree_top + 1):
            factor = math.sqrt(
                (2 * degree + 1)
                / (4.0 * math.pi)
                * math.factorial(degree - azimuthal)
                / math.factorial(degree + azimuthal)
            )
            if azimuthal == 0:
                results[degree, 0] = factor * legendre[degree]
            else:
                results[degree, azimuthal] = (
                    math.sqrt(2.0) * factor * legendre[degree] * real_part[azimuthal]
                )
                results[degree, -azimuthal] = (
                    math.sqrt(2.0) * factor * legendre[degree] * imag_part[azimuthal]
                )
    return results


def kept_rows():
    row_list = [(degree, 0) for degree in range(LMAX + 1)]
    for azimuthal in range(1, MMAX + 1):
        row_list += [(degree, azimuthal) for degree in range(azimuthal, LMAX + 1)]
        row_list += [(degree, -azimuthal) for degree in range(azimuthal, LMAX + 1)]
    return row_list


def row_offsets():
    listing = []
    offset = 0
    for degree, azimuthal in kept_rows():
        listing.append((degree, offset))
        offset += 2 * degree + 1
    return listing


def invert_small(matrix):
    order_size = matrix.shape[0]
    work = np.concatenate([matrix, np.eye(order_size)], axis=1)
    for column in range(order_size):
        work[column] = work[column] / work[column, column]
        for row_index in range(order_size):
            if row_index != column:
                work[row_index] = work[row_index] - work[row_index, column] * work[column]
    return work[:, order_size:]


def sample_tables():
    sample_count = 2 * (LMAX + 1) ** 2
    positions = np.arange(sample_count) + 0.5
    height = 1.0 - 2.0 * positions / sample_count
    radius = np.sqrt(1.0 - height * height)
    azimuth = math.pi * (3.0 - math.sqrt(5.0)) * positions
    points = np.stack([radius * np.cos(azimuth), radius * np.sin(azimuth), height])
    values = harmonics(points[0], points[1], points[2], LMAX, LMAX)
    inverses = []
    for degree in range(LMAX + 1):
        sampled = np.stack([values[degree, azimuthal] for azimuthal in range(-degree, degree + 1)])
        inverses.append(sampled.T @ invert_small(sampled @ sampled.T))
    return (points, inverses)


def wigner_rows(vectors):
    length = jnp.sqrt(jnp.sum(vectors * vectors, axis=0))
    direction = vectors / length
    pick_first = jnp.where(jnp.abs(direction[0]) < 0.6, 1.0, 0.0).astype(jnp.float32)
    helper = jnp.stack([pick_first, 1.0 - pick_first, jnp.zeros_like(pick_first)])
    first_axis = jnp.cross(direction, helper, axis=0)
    first_axis = first_axis / jnp.sqrt(jnp.sum(first_axis * first_axis, axis=0))
    second_axis = jnp.cross(direction, first_axis, axis=0)
    frames = jnp.stack([first_axis, second_axis, direction])
    points, inverses = sample_tables()
    sample = jnp.asarray(points, jnp.float32)
    turned = jnp.einsum("rce,ck->rek", frames, sample, precision=highest)
    values = harmonics(turned[0], turned[1], turned[2], LMAX, MMAX)
    pieces = []
    for degree, azimuthal in kept_rows():
        table = jnp.asarray(inverses[degree], jnp.float32)
        pieces.append(jnp.dot(values[degree, azimuthal], table, precision=highest))
    compact = jnp.concatenate(pieces, axis=1)
    envelope = 0.5 * (jnp.cos(math.pi * length / cutoff_radius) + 1.0)
    return (compact, envelope)


def one_hot(indices, width):
    return (indices[:, None] == jnp.arange(width, dtype=jnp.int32)[None, :]).astype(jnp.bfloat16)


def rotate_forward(compact_t, scaling, sources):
    rows_out = []
    for degree, offset in row_offsets():
        span = 2 * degree + 1
        total = None
        for inner in range(span):
            term = compact_t[offset + inner].astype(jnp.float32)[None, :] * sources[
                degree * degree + inner
            ].astype(jnp.float32)
            total = term if total is None else total + term
        rows_out.append(total * scaling[None, :])
    return jnp.stack(rows_out, axis=0).astype(jnp.bfloat16)


def convolve(turned, weight_zero, weight_one, weight_two):
    end_zero = LMAX + 1
    end_one_plus = end_zero + LMAX
    end_one_minus = end_one_plus + LMAX
    end_two_plus = end_one_minus + LMAX - 1
    zero_part = turned[:end_zero]
    one_plus = turned[end_zero:end_one_plus]
    one_minus = turned[end_one_plus:end_one_minus]
    two_plus = turned[end_one_minus:end_two_plus]
    two_minus = turned[end_two_plus:]

    def contract(parts, weight, rows):
        left = jnp.concatenate(parts, axis=0)
        edges = left.shape[-1]
        left = left.reshape(-1, edges)
        right = weight.reshape(left.shape[0], -1)
        out = lax.dot_general(
            left, right, (((0,), (0,)), ((), ())), preferred_element_type=jnp.float32
        ).astype(jnp.bfloat16)
        return [out[:, row * 256 : (row + 1) * 256] for row in range(rows)]

    return (
        contract([zero_part], weight_zero, LMAX + 1)
        + contract([one_plus, -one_minus], weight_one, LMAX)
        + contract([one_minus, one_plus], weight_one, LMAX)
        + contract([two_plus, -two_minus], weight_two, LMAX - 1)
        + contract([two_minus, two_plus], weight_two, LMAX - 1)
    )


def shards(
    node_states,
    edge_vectors,
    source_part,
    source_slot,
    target_slot,
    live_edges,
    weight_zero,
    weight_one,
    weight_two,
):
    slab_size = source_slot.shape[0]
    local_nodes = node_states.shape[0]
    local_channels = node_states.shape[2]
    coef_count = node_states.shape[1]
    group_count = lax.axis_size("edge")
    node_flat = node_states.reshape(local_nodes, coef_count * local_channels)
    table = lax.all_gather(node_flat, "edge", axis=0, tiled=True)
    quarter, quarter_fade = wigner_rows(edge_vectors)
    packed = jnp.concatenate([quarter, quarter_fade[:, None]], axis=1).astype(jnp.bfloat16)
    packed_t = lax.all_gather(packed, "chan", axis=0, tiled=True).T
    compact_t, envelope = packed_t[:-1], packed_t[-1]
    alive_mask = (jnp.arange(slab_size, dtype=jnp.int32) < live_edges[0]).astype(jnp.float32)
    scaling = envelope.astype(jnp.float32) * alive_mask
    source = source_part[:, 0] * local_nodes + source_slot
    select = one_hot(source, group_count * local_nodes)
    sources = (
        lax.dot_general(
            table, select, (((0,), (1,)), ((), ())), preferred_element_type=jnp.float32
        )
        .astype(jnp.bfloat16)
        .reshape(coef_count, local_channels, slab_size)
    )
    turned = rotate_forward(compact_t, scaling, sources)
    mixed = convolve(turned, weight_zero, weight_one, weight_two)
    selector = (jnp.arange(local_nodes, dtype=jnp.int32)[:, None] == target_slot[None, :]).astype(
        jnp.bfloat16
    )
    listing = row_offsets()
    sums = []
    for degree in range(LMAX + 1):
        span = 2 * degree + 1
        picked_rows = [
            (row, offset) for row, (row_degree, offset) in enumerate(listing) if row_degree == degree
        ]
        left = jnp.concatenate(
            [
                (compact_t[offset : offset + span][None] * selector[:, None]).reshape(
                    local_nodes * span, slab_size
                )
                for row, offset in picked_rows
            ],
            axis=1,
        )
        right = jnp.concatenate([mixed[row] for row, offset in picked_rows], axis=0)
        sums.append(
            jnp.dot(left, right, preferred_element_type=jnp.float32).reshape(
                local_nodes, span, -1
            )
        )
    partial = jnp.concatenate(sums, axis=1).astype(jnp.bfloat16)
    return lax.psum_scatter(partial, "chan", scatter_dimension=2, tiled=True)


def solution(mesh):
    in_specs = (
        P("edge", None, "chan"),
        P(None, ("edge", "chan")),
        P("edge", None),
        P("edge"),
        P("edge"),
        P("edge"),
        P(None, "chan", None, None),
        P(None, None, "chan", None, None),
        P(None, None, "chan", None, None),
    )
    out_specs = P("edge", None, "chan")
    return jax.shard_map(shards, mesh=mesh, in_specs=in_specs, out_specs=out_specs, check_vma=False)
```

```python
import math

import jax
import jax.numpy as jnp
import numpy as np
from jax import lax
from jax.experimental import pallas as pl
from jax.experimental.pallas import tpu as pltpu
from jax.sharding import PartitionSpec as P

LMAX = 6
MMAX = 2
COEFS = (LMAX + 1) ** 2
CUTOFF = 6.0
LANES = 128
MESH = pl.DeviceIdType.MESH

Y_RING, Z_RING = 4, 8
HALVES = {"A": ((0, 5), (5, 10)), "B": ((10, 18), (18, 25))}


def schedule():
    step = {"y+": (1, 0), "y-": (-1, 0), "z+": (0, 1), "z-": (0, -1)}
    free = {link: 0.0 for link in step}
    waiting = {link: [] for link in step}
    events = [(4.0, 0, "A", (0, 1), 0, 0, ""), (4.0, 1, "B", (0, 1), 0, 0, "")]
    count = 2
    sends = []

    def follow(colour, half, oy, oz, via):
        first, second = ("y", "z") if colour == "A" else ("z", "y")
        offset = {"y": oy, "z": oz}
        limit = {"y": Y_RING // 2, "z": Z_RING // 2}
        routes = []

        def along(axis, rank):
            moved = offset[axis]
            for sign, mine in (("+", 0), ("-", 1)):
                if moved != 0 and via != axis + sign:
                    continue
                hops = abs(moved) + 1
                if hops > limit[axis]:
                    continue
                taken = (mine,) if hops == limit[axis] else half
                taken = tuple(h for h in taken if h in half)
                if taken:
                    routes.append((rank + limit[axis] - hops, axis + sign, taken))

        if offset[second] == 0:
            along(first, 10)
        along(second, 0)
        return routes

    while events or any(waiting.values()):
        ready = [
            (max(free[link], min(item[0] for item in items)), link)
            for link, items in waiting.items()
            if items
        ]
        begin = min(ready) if ready else None
        if events and (begin is None or min(events)[0] <= begin[0]):
            event = min(events)
            events.remove(event)
            time, _, colour, half, oy, oz, via = event
            for rank, link, taken in follow(colour, half, oy, oz, via):
                waiting[link].append((time, -rank, count, colour, taken, oy, oz))
                count += 1
            continue
        time, link = begin
        items = [item for item in waiting[link] if item[0] <= time]
        item = min(items, key=lambda it: (it[1], it[0], it[2]))
        waiting[link].remove(item)
        _, _, _, colour, half, oy, oz = item
        tiles = [HALVES[colour][h] for h in half]
        first, end = tiles[0][0], tiles[-1][1]
        free[link] = time + (end - first) * 2 * 4096 / 46.6e3
        dy, dz = step[link]
        sends.append((time, link, first, end, oy, oz))
        events.append((free[link] + 1.8, count, colour, half, oy - dy, oz - dz, link))
        count += 1
    return [send[1:] for send in sorted(sends)]


SENDS = schedule()
STEP = {"y+": (1, 0), "y-": (-1, 0), "z+": (0, 1), "z-": (0, -1)}
TILES = 25


def harmonics_at(points, degree_top):
    x, y, z = points
    rows = {}
    real, imag = [np.ones_like(x)], [np.zeros_like(x)]
    for m in range(1, degree_top + 1):
        real.append(x * real[m - 1] - y * imag[m - 1])
        imag.append(x * imag[m - 1] + y * real[m - 1])
    for m in range(degree_top + 1):
        start = (-1.0) ** m * math.prod(range(2 * m - 1, 0, -2))
        legendre = {m: np.full_like(z, start), m + 1: z * ((2 * m + 1) * start)}
        for l in range(m + 2, degree_top + 1):
            legendre[l] = (
                (2 * l - 1) * z * legendre[l - 1] - (l + m - 1) * legendre[l - 2]
            ) / (l - m)
        for l in range(m, degree_top + 1):
            factor = math.sqrt(
                (2 * l + 1) / (4 * math.pi) * math.factorial(l - m) / math.factorial(l + m)
            )
            if m == 0:
                rows[l, 0] = factor * legendre[l]
            else:
                rows[l, m] = math.sqrt(2.0) * factor * legendre[l] * real[m]
                rows[l, -m] = math.sqrt(2.0) * factor * legendre[l] * imag[m]
    return np.stack([rows[l, m] for l in range(degree_top + 1) for m in range(-l, l + 1)])


def raising_tables():
    count = 4 * (LMAX + 2) ** 2
    at = np.arange(count) + 0.5
    height = 1.0 - 2.0 * at / count
    radius = np.sqrt(1.0 - height * height)
    angle = math.pi * (3.0 - math.sqrt(5.0)) * at
    points = np.stack([radius * np.cos(angle), radius * np.sin(angle), height])
    basis = harmonics_at(points, LMAX)
    inverse = np.linalg.pinv(basis.T)
    tables = {}
    for l in range(1, LMAX + 1):
        below = basis[(l - 1) ** 2 : l * l]
        tables[l] = [
            np.where(np.abs(part) < 1e-9, 0.0, part)
            for part in (
                (inverse @ (points[c] * below).T)[l * l : (l + 1) ** 2] for c in range(3)
            )
        ]
    return tables


RAISE = raising_tables()


def project(table, degree, weights, rows):
    results = []
    for m in range(2 * degree + 1):
        total = None
        for axis in range(3):
            for n in range(2 * degree - 1):
                value = float(table[axis][m, n])
                if value != 0.0:
                    term = (value * weights[axis]) * rows[n]
                    total = term if total is None else total + term
        results.append(total)
    return results


def wigner_into(rot_ref, vectors):
    x, y, z = vectors[0:1], vectors[1:2], vectors[2:3]
    length = jnp.sqrt(x * x + y * y + z * z)
    u = [x / length, y / length, z / length]
    pick = jnp.where(jnp.abs(u[0]) < 0.6, 1.0, 0.0)
    other = 1.0 - pick
    a = [-u[2] * other, u[2] * pick, u[0] * other - u[1] * pick]
    norm = jnp.sqrt(a[0] * a[0] + a[1] * a[1] + a[2] * a[2])
    a = [part / norm for part in a]
    b = [
        u[1] * a[2] - u[2] * a[1],
        u[2] * a[0] - u[0] * a[2],
        u[0] * a[1] - u[1] * a[0],
    ]
    shape = (8, x.shape[1])
    order = lax.broadcasted_iota(jnp.int32, shape, 0)
    wide = [jnp.broadcast_to(part, shape) for part in u]
    below = [jnp.where(order == 0, 1.0, 0.0)]
    rot_ref[0] = below[0]
    for l in range(1, LMAX + 1):
        table = RAISE[l]
        inverse = [1.0 / float(table[2][m + l, m + l - 1]) if m < l else 0.0 for m in range(3)]
        scale = jnp.where(
            order == 0, inverse[0], jnp.where(order <= 2, inverse[1], inverse[2])
        )
        rows = project(table, l, [part * scale for part in wide], below)
        rows = [jnp.zeros(shape, jnp.float32) if row is None else row for row in rows]
        if l == 1:
            first = project(table, 1, a, [1.0])
            second = project(table, 1, b, [1.0])
            one = 1.0 / float(table[0][2, 0])
            two = 1.0 / float(table[1][0, 0])
            rows = [
                jnp.where(order == 1, one * f, jnp.where(order == 2, two * s, r))
                for f, s, r in zip(first, second, rows)
            ]
        if l == 2:
            plus = [row[1:2] for row in below]
            minus = [row[2:3] for row in below]
            aa, bb = project(table, 2, a, plus), project(table, 2, b, minus)
            ab, ba = project(table, 2, a, minus), project(table, 2, b, plus)
            one = 1.0 / float(table[0][4, 2] - table[1][4, 0])
            two = 1.0 / float(table[0][0, 0] + table[1][0, 2])
            rows = [
                jnp.where(
                    order == 3,
                    one * (aa[m] - bb[m]),
                    jnp.where(order == 4, two * (ab[m] + ba[m]), rows[m]),
                )
                for m in range(5)
            ]
        for k, row in enumerate(rows):
            rot_ref[l * l + k] = row
        below = rows
    return length


def gather_kernel(block_ref, vector_ref, table_ref, vectors_ref, send, recv, xsem, vsem, own):
    edge = lax.axis_index("edge")
    chan = lax.axis_index("chan")
    x = edge % 2
    z = (edge // 2) % Z_RING
    y = edge // (2 * Z_RING)

    def at(oy, oz, side=0):
        row = (y + (oy + Y_RING)) % Y_RING
        column = (z + (oz + Z_RING)) % Z_RING
        return (row * Z_RING + column) * 2 + side

    partner = at(0, 0, 1 - x)
    neighbours = {link: at(dy, dz, x) for link, (dy, dz) in STEP.items()}
    barrier = pltpu.get_barrier_semaphore()
    for target in [partner, *neighbours.values()]:
        pl.semaphore_signal(
            barrier, inc=1, device_id={"edge": target, "chan": chan}, device_id_type=MESH
        )
    for far in range(1, 4):
        pl.semaphore_signal(
            barrier,
            inc=1,
            device_id={"edge": edge, "chan": (chan + far) % 4},
            device_id_type=MESH,
        )
    mine = pltpu.make_async_copy(block_ref, table_ref.at[edge], own.at[0])
    mine.start()
    vector = pltpu.make_async_copy(vector_ref, vectors_ref.at[chan], own.at[1])
    vector.start()
    pl.semaphore_wait(barrier, 8)
    across = pltpu.make_async_remote_copy(
        src_ref=block_ref,
        dst_ref=table_ref.at[edge],
        send_sem=xsem.at[0],
        recv_sem=xsem.at[1],
        device_id={"edge": partner, "chan": chan},
        device_id_type=MESH,
    )
    across.start()
    spread = []
    for far in range(1, 4):
        copy = pltpu.make_async_remote_copy(
            src_ref=vector_ref,
            dst_ref=vectors_ref.at[chan],
            send_sem=vsem.at[far - 1],
            recv_sem=vsem.at[far + 2],
            device_id={"edge": edge, "chan": (chan + far) % 4},
            device_id_type=MESH,
        )
        copy.start()
        spread.append(copy)
    mine.wait()
    vector.wait()
    across.wait_recv()
    copies, landed = [], []
    for index, (link, first, end, oy, oz) in enumerate(SENDS):
        dy, dz = STEP[link]
        view = table_ref.at[pl.ds(at(oy, oz), 2), pl.ds(first, end - first)]
        copies.append(
            pltpu.make_async_remote_copy(
                src_ref=view,
                dst_ref=view,
                send_sem=send.at[index],
                recv_sem=recv.at[index],
                device_id={"edge": neighbours[link], "chan": chan},
                device_id_type=MESH,
            )
        )
        landed.append((first, end, (oy - dy) % Y_RING, (oz - dz) % Z_RING))
    waited = set()
    for index, (link, first, end, oy, oz) in enumerate(SENDS):
        for other, (begin, stop, ry, rz) in enumerate(landed):
            if (
                other not in waited
                and (ry, rz) == (oy % Y_RING, oz % Z_RING)
                and begin < end
                and first < stop
            ):
                copies[other].wait_recv()
                waited.add(other)
        copies[index].start()
    for index, copy in enumerate(copies):
        if index not in waited:
            copy.wait_recv()
    for copy in spread:
        copy.wait()
    across.wait_send()
    for copy in copies:
        copy.wait_send()


def gather(block, vector):
    return pl.pallas_call(
        gather_kernel,
        name="gather_table",
        out_shape=(
            jax.ShapeDtypeStruct((64, *block.shape), block.dtype),
            jax.ShapeDtypeStruct((4, *vector.shape), vector.dtype),
        ),
        in_specs=[pl.BlockSpec(memory_space=pltpu.VMEM)] * 2,
        out_specs=[pl.BlockSpec(memory_space=pltpu.VMEM)] * 2,
        scratch_shapes=[
            pltpu.SemaphoreType.DMA((len(SENDS),)),
            pltpu.SemaphoreType.DMA((len(SENDS),)),
            pltpu.SemaphoreType.DMA((2,)),
            pltpu.SemaphoreType.DMA((6,)),
            pltpu.SemaphoreType.DMA((2,)),
        ],
        compiler_params=pltpu.CompilerParams(
            collective_id=0, has_side_effects=True, vmem_limit_bytes=40 << 20
        ),
    )(block, vector)


STARTS = {"p1": 0, "n1": 768, "p2": 1536, "n2": 2176, "z": 2816}
LEFT_BLOCKS = 26


def left_rows(order, degree):
    if order == 0:
        return [(STARTS["z"] + 64 * degree, False)]
    m = (order + 1) // 2
    count = LMAX + 1 - m
    plus, minus = STARTS["p%d" % m], STARTS["n%d" % m]
    here = 64 * (degree - m)
    if order % 2:
        return [(plus + here, False), (minus + 64 * count + here, False)]
    return [(minus + here, False), (plus + 64 * count + here, True)]


def coefficient_row(k):
    return (k % TILES) * LANES + (k // TILES) * 64


def layer_kernel(
    table_ref,
    vectors_ref,
    source_ref,
    target_ref,
    live_ref,
    zero_hbm,
    one_hbm,
    two_hbm,
    out_ref,
    zero_ref,
    one_ref,
    two_ref,
    rot_ref,
    pick_ref,
    states_ref,
    rows_ref,
    left_ref,
    sum_ref,
    sems,
):
    loads = [
        pltpu.make_async_copy(src, dst, sems.at[index])
        for index, (src, dst) in enumerate(
            ((one_hbm, one_ref), (two_hbm, two_ref), (zero_hbm, zero_ref))
        )
    ]
    for load in loads:
        load.start()
    edges = source_ref.shape[1]
    vectors = jnp.concatenate([vectors_ref[part] for part in range(4)], axis=1)
    length = wigner_into(rot_ref, vectors)
    alive = lax.broadcasted_iota(jnp.int32, (1, edges), 1) < live_ref[0]
    scaling = jnp.where(alive, 0.5 * (jnp.cos(length * (math.pi / CUTOFF)) + 1.0), 0.0)
    source = jnp.broadcast_to(source_ref[...].astype(jnp.float32), (LANES, edges)).T
    lane = lax.broadcasted_iota(jnp.int32, (edges, LANES), 1).astype(jnp.float32)
    for part in range(8):
        pick_ref[:, part * LANES : (part + 1) * LANES] = jnp.where(
            source == lane + float(part * LANES), 1.0, 0.0
        ).astype(jnp.bfloat16)

    def pick_pair(first, count):
        right = [
            table_ref[:, first + step].reshape(1024, LANES) for step in range(count)
        ]
        right = right[0] if count == 1 else jnp.concatenate(right, axis=1)
        picked = jnp.dot(pick_ref[...], right, preferred_element_type=jnp.float32)
        rows = pl.ds(pl.multiple_of(first * LANES, LANES), count * LANES)
        states_ref[rows, :] = picked.astype(jnp.bfloat16).T

    def pick_step(step, carry):
        pick_pair(step * 2, 2)
        return carry

    lax.fori_loop(0, 12, pick_step, 0)
    pick_pair(24, 1)

    scale = jnp.broadcast_to(scaling, (16, edges))
    for degree in range(LMAX + 1):
        orders = min(2 * min(degree, MMAX) + 1, 5)
        base = degree * degree

        def turn(chunk, carry, degree=degree, orders=orders, base=base):
            start = pl.multiple_of(chunk * 16, 16)
            totals = [None] * orders
            for k in range(2 * degree + 1):
                rows = pl.ds(coefficient_row(base + k) + start, 16)
                value = states_ref[rows, :].astype(jnp.float32)
                for order in range(orders):
                    factor = rot_ref[base + k, order : order + 1, :]
                    term = factor * value
                    totals[order] = term if k == 0 else totals[order] + term
            for order in range(orders):
                result = totals[order] * scale
                for first, negate in left_rows(order, degree):
                    rows_ref[pl.ds(first + start, 16), :] = (
                        -result if negate else result
                    ).astype(jnp.bfloat16)
            return carry

        lax.fori_loop(0, 4, turn, 0)

    def flip(block, carry):
        rows = pl.ds(pl.multiple_of(block * LANES, LANES), LANES)
        left_ref[block] = rows_ref[rows, :].T
        return carry

    lax.fori_loop(0, LEFT_BLOCKS, flip, 0)
    sum_ref[...] = jnp.zeros_like(sum_ref)
    slot = lax.broadcasted_iota(jnp.int32, (16, edges), 0)
    chosen = jnp.where(slot == target_ref[...], 1.0, 0.0)

    def left(first, depth):
        blocks = [left_ref[first // LANES + i] for i in range(-(-depth // LANES))]
        whole = jnp.concatenate(blocks, axis=1)
        return whole[:, :depth]

    def mix(order, degree, start, depth, right):
        mixed = jnp.dot(left(start, depth), right, preferred_element_type=jnp.float32)
        mixed = mixed.astype(jnp.bfloat16)
        back = jnp.concatenate(
            [
                (rot_ref[degree * degree + k, order : order + 1, :] * chosen).astype(jnp.bfloat16)
                for k in range(2 * degree + 1)
            ],
            axis=0,
        )
        rows = pl.ds(16 * degree * degree, 16 * (2 * degree + 1))
        sum_ref[rows, :] += jnp.dot(back, mixed, preferred_element_type=jnp.float32)

    loads[0].wait()
    for degree in range(1, LMAX + 1):
        right = one_ref[:, :, degree - 1].reshape(768, 256)
        mix(1, degree, STARTS["p1"], 768, right)
        mix(2, degree, STARTS["n1"], 768, right)
    loads[1].wait()
    for degree in range(2, LMAX + 1):
        right = two_ref[:, :, degree - 2].reshape(640, 256)
        mix(3, degree, STARTS["p2"], 640, right)
        mix(4, degree, STARTS["n2"], 640, right)
    loads[2].wait()
    for degree in range(LMAX + 1):
        right = zero_ref[:, degree].reshape(448, 256)
        mix(0, degree, STARTS["z"], 448, right)
    for part in range(4):
        lanes = pl.ds(64 * part, 64)
        out_ref[part] = jnp.concatenate(
            [sum_ref[0:400, lanes], sum_ref[400:800, lanes]], axis=1
        ).astype(jnp.bfloat16)


def layer(table, vectors, source, target, live, zero, one, two):
    edges = source.shape[1]
    vmem = pl.BlockSpec(memory_space=pltpu.VMEM)
    hbm = pl.BlockSpec(memory_space=pl.ANY)
    return pl.pallas_call(
        layer_kernel,
        name="layer",
        out_shape=jax.ShapeDtypeStruct((4, 400, LANES), jnp.bfloat16),
        in_specs=[vmem, vmem, vmem, vmem, pl.BlockSpec(memory_space=pltpu.SMEM), hbm, hbm, hbm],
        out_specs=vmem,
        scratch_shapes=[
            pltpu.VMEM(zero.shape, jnp.bfloat16),
            pltpu.VMEM(one.shape, jnp.bfloat16),
            pltpu.VMEM(two.shape, jnp.bfloat16),
            pltpu.VMEM((COEFS, 8, edges), jnp.float32),
            pltpu.VMEM((edges, 1024), jnp.bfloat16),
            pltpu.VMEM((TILES * LANES, edges), jnp.bfloat16),
            pltpu.VMEM((LEFT_BLOCKS * LANES, edges), jnp.bfloat16),
            pltpu.VMEM((LEFT_BLOCKS, edges, LANES), jnp.bfloat16),
            pltpu.VMEM((800, 256), jnp.float32),
            pltpu.SemaphoreType.DMA((3,)),
        ],
        compiler_params=pltpu.CompilerParams(vmem_limit_bytes=60 << 20),
    )(table, vectors, source, target, live, zero, one, two)


def reduce_kernel(parts_ref, out_ref, landing, send, recv):
    edge = lax.axis_index("edge")
    chan = lax.axis_index("chan")
    barrier = pltpu.get_barrier_semaphore()
    for far in range(1, 4):
        pl.semaphore_signal(
            barrier,
            inc=1,
            device_id={"edge": edge, "chan": (chan + far) % 4},
            device_id_type=MESH,
        )
    pl.semaphore_wait(barrier, 3)
    copies = []
    for far in (2, 1, 3):
        target = (chan + far) % 4
        copy = pltpu.make_async_remote_copy(
            src_ref=parts_ref.at[target],
            dst_ref=landing.at[far - 1],
            send_sem=send.at[far - 1],
            recv_sem=recv.at[far - 1],
            device_id={"edge": edge, "chan": target},
            device_id_type=MESH,
        )
        copy.start()
        copies.append(copy)
    for copy in copies:
        copy.wait_recv()
    total = parts_ref[chan].astype(jnp.float32)
    for slot in range(3):
        total = total + landing[slot].astype(jnp.float32)
    out_ref[...] = total.astype(jnp.bfloat16)
    for copy in copies:
        copy.wait_send()


def reduce(parts):
    return pl.pallas_call(
        reduce_kernel,
        name="reduce_parts",
        out_shape=jax.ShapeDtypeStruct(parts.shape[1:], parts.dtype),
        in_specs=[pl.BlockSpec(memory_space=pltpu.VMEM)],
        out_specs=pl.BlockSpec(memory_space=pltpu.VMEM),
        scratch_shapes=[
            pltpu.VMEM((3, *parts.shape[1:]), parts.dtype),
            pltpu.SemaphoreType.DMA((3,)),
            pltpu.SemaphoreType.DMA((3,)),
        ],
        compiler_params=pltpu.CompilerParams(collective_id=1, has_side_effects=True),
    )(parts)


def shards(
    node_states,
    edge_vectors,
    source_part,
    source_slot,
    target_slot,
    live_edges,
    weight_zero,
    weight_one,
    weight_two,
):
    nodes = node_states.transpose(1, 0, 2)
    block = jnp.concatenate(
        [nodes[:TILES], jnp.pad(nodes[TILES:], ((0, 1), (0, 0), (0, 0)))], axis=2
    )
    vector = jnp.pad(edge_vectors, ((0, 5), (0, 0)))
    table, vectors = gather(block, vector)
    source = (source_part[:, 0] * node_states.shape[0] + source_slot)[None, :]
    parts = layer(
        table,
        vectors,
        source,
        target_slot[None, :],
        live_edges,
        weight_zero.transpose(0, 2, 1, 3),
        weight_one.transpose(0, 1, 3, 2, 4),
        weight_two.transpose(0, 1, 3, 2, 4),
    )
    total = reduce(parts).reshape(TILES, 16, LANES)
    result = jnp.concatenate([total[:, :, :64], total[: COEFS - TILES, :, 64:]], axis=0)
    return result.transpose(1, 0, 2)


def solution(mesh):
    in_specs = (
        P("edge", None, "chan"),
        P(None, ("edge", "chan")),
        P("edge", None),
        P("edge"),
        P("edge"),
        P("edge"),
        P(None, "chan", None, None),
        P(None, None, "chan", None, None),
        P(None, None, "chan", None, None),
    )
    out_specs = P("edge", None, "chan")
    return jax.shard_map(shards, mesh=mesh, in_specs=in_specs, out_specs=out_specs, check_vma=False)
```

```python
import math

import jax
import jax.numpy as jnp
import numpy as np
from jax import lax
from jax.experimental import pallas as pl
from jax.experimental.pallas import tpu as pltpu
from jax.sharding import PartitionSpec as P

LMAX = 6
MMAX = 2
COEFS = (LMAX + 1) ** 2
CUTOFF = 6.0
LANES = 128
TILES = 25
MESH = pl.DeviceIdType.MESH

Y_RING, Z_RING = 4, 8
STEP = {"y+": (1, 0), "y-": (-1, 0), "z+": (0, 1), "z-": (0, -1), "x": (0, 0)}
COLOURS = {
    "py": ("y", True, ((0, 3), (3, 6))),
    "sy": ("y", False, ((6, 8), (8, 10))),
    "pz": ("z", True, ((10, 15), (15, 19))),
    "sz": ("z", False, ((19, 22), (22, 25))),
}
Y_TILES = 10
LATENCY, BYTES_PER_US, BLOCK_TILE = 1.8, 46.6e3, 4096


def schedule():
    free = {link: 0.0 for link in STEP}
    waiting = {link: [] for link in STEP}
    events, sends, begun, landed = [], [], [], []
    count = 0

    def put(link, time, rank, colour, half, oy, oz):
        nonlocal count
        waiting[link].append((time, -rank, count, colour, half, oy, oz))
        count += 1

    def follow(time, colour, half, oy, oz, via):
        axis_first, paired, _ = COLOURS[colour]
        if via == "x" and not paired:
            return
        via = "" if via == "x" else via
        if not paired:
            put("x", time, 0, colour, half, oy, oz)
        second = "z" if axis_first == "y" else "y"
        offset = {"y": oy, "z": oz}
        limit = {"y": Y_RING // 2, "z": Z_RING // 2}

        def along(axis, rank):
            moved = offset[axis]
            for sign, mine in (("+", 0), ("-", 1)):
                hops = abs(moved) + 1
                if (moved != 0 and via != axis + sign) or hops > limit[axis]:
                    continue
                taken = (mine,) if hops == limit[axis] else half
                taken = tuple(h for h in taken if h in half)
                if taken:
                    put(axis + sign, time, rank + limit[axis] - hops, colour, taken, oy, oz)

        if offset[second] == 0:
            along(axis_first, 10)
        along(second, 0)

    for colour, (_, paired, _) in COLOURS.items():
        if paired:
            put("x", 0.0, 20, colour, (0, 1), 0, 0)
        else:
            follow(0.0, colour, (0, 1), 0, 0, "")
    while events or any(waiting.values()):
        ready = [
            (max(free[link], min(item[0] for item in items)), link)
            for link, items in waiting.items()
            if items
        ]
        begin = min(ready) if ready else None
        if events and (begin is None or min(events)[0] <= begin[0]):
            event = min(events)
            events.remove(event)
            time, _, colour, half, oy, oz, via = event
            follow(time, colour, half, oy, oz, via)
            continue
        time, link = begin
        item = min(
            (item for item in waiting[link] if item[0] <= time),
            key=lambda it: (it[1], it[0], it[2]),
        )
        waiting[link].remove(item)
        known, _, _, colour, half, oy, oz = item
        _, paired, halves = COLOURS[colour]
        first, end = halves[half[0]][0], halves[half[-1]][1]
        both = paired and link != "x"
        free[link] = time + (end - first) * (2 if both else 1) * BLOCK_TILE / BYTES_PER_US
        earlier = [b for b, s in zip(begun, sends) if s[0] == link]
        dy, dz = STEP[link]
        sends.append((link, both, first, end, oy, oz))
        begun.append(max([known] + earlier[-1:]))
        landed.append(free[link] + LATENCY)
        events.append((landed[-1], count, colour, half, oy - dy, oz - dz, link))
        count += 1
    steps = [(time, 1, index, "send") for index, time in enumerate(begun)]
    steps += [(time, 0, index, "wait") for index, time in enumerate(landed)]
    return sends, [(kind, index) for _, _, index, kind in sorted(steps)]


SENDS, PROGRAM = schedule()


def brought(index):
    link, both, first, end, oy, oz = SENDS[index]
    dy, dz = STEP[link]
    sides = ("own", "other") if both else (("other",) if link == "x" else ("own",))
    return {
        (tile, (oy - dy) % Y_RING, (oz - dz) % Z_RING, side)
        for tile in range(first, end)
        for side in sides
    }


def harmonics_at(points, degree_top):
    x, y, z = points
    rows = {}
    real, imag = [np.ones_like(x)], [np.zeros_like(x)]
    for m in range(1, degree_top + 1):
        real.append(x * real[m - 1] - y * imag[m - 1])
        imag.append(x * imag[m - 1] + y * real[m - 1])
    for m in range(degree_top + 1):
        start = (-1.0) ** m * math.prod(range(2 * m - 1, 0, -2))
        legendre = {m: np.full_like(z, start), m + 1: z * ((2 * m + 1) * start)}
        for l in range(m + 2, degree_top + 1):
            legendre[l] = (
                (2 * l - 1) * z * legendre[l - 1] - (l + m - 1) * legendre[l - 2]
            ) / (l - m)
        for l in range(m, degree_top + 1):
            factor = math.sqrt(
                (2 * l + 1) / (4 * math.pi) * math.factorial(l - m) / math.factorial(l + m)
            )
            if m == 0:
                rows[l, 0] = factor * legendre[l]
            else:
                rows[l, m] = math.sqrt(2.0) * factor * legendre[l] * real[m]
                rows[l, -m] = math.sqrt(2.0) * factor * legendre[l] * imag[m]
    return np.stack([rows[l, m] for l in range(degree_top + 1) for m in range(-l, l + 1)])


def raising_tables():
    count = 4 * (LMAX + 2) ** 2
    at = np.arange(count) + 0.5
    height = 1.0 - 2.0 * at / count
    radius = np.sqrt(1.0 - height * height)
    angle = math.pi * (3.0 - math.sqrt(5.0)) * at
    points = np.stack([radius * np.cos(angle), radius * np.sin(angle), height])
    basis = harmonics_at(points, LMAX)
    inverse = np.linalg.pinv(basis.T)
    tables = {}
    for l in range(1, LMAX + 1):
        below = basis[(l - 1) ** 2 : l * l]
        tables[l] = [
            np.where(np.abs(part) < 1e-9, 0.0, part)
            for part in (
                (inverse @ (points[c] * below).T)[l * l : (l + 1) ** 2] for c in range(3)
            )
        ]
    return tables


RAISE = raising_tables()


def project(table, degree, weights, rows):
    results = []
    for m in range(2 * degree + 1):
        total = None
        for axis in range(3):
            for n in range(2 * degree - 1):
                value = float(table[axis][m, n])
                if value != 0.0:
                    term = (value * weights[axis]) * rows[n]
                    total = term if total is None else total + term
        results.append(total)
    return results


def wigner_into(rot_ref, vectors):
    x, y, z = vectors[0:1], vectors[1:2], vectors[2:3]
    length = jnp.sqrt(x * x + y * y + z * z)
    u = [x / length, y / length, z / length]
    pick = jnp.where(jnp.abs(u[0]) < 0.6, 1.0, 0.0)
    other = 1.0 - pick
    a = [-u[2] * other, u[2] * pick, u[0] * other - u[1] * pick]
    norm = jnp.sqrt(a[0] * a[0] + a[1] * a[1] + a[2] * a[2])
    a = [part / norm for part in a]
    b = [
        u[1] * a[2] - u[2] * a[1],
        u[2] * a[0] - u[0] * a[2],
        u[0] * a[1] - u[1] * a[0],
    ]
    shape = (8, x.shape[1])
    order = lax.broadcasted_iota(jnp.int32, shape, 0)
    wide = [jnp.broadcast_to(part, shape) for part in u]
    below = [jnp.where(order == 0, 1.0, 0.0)]
    rot_ref[0] = below[0]
    for l in range(1, LMAX + 1):
        table = RAISE[l]
        inverse = [1.0 / float(table[2][m + l, m + l - 1]) if m < l else 0.0 for m in range(3)]
        scale = jnp.where(
            order == 0, inverse[0], jnp.where(order <= 2, inverse[1], inverse[2])
        )
        rows = project(table, l, [part * scale for part in wide], below)
        rows = [jnp.zeros(shape, jnp.float32) if row is None else row for row in rows]
        if l == 1:
            first = project(table, 1, a, [1.0])
            second = project(table, 1, b, [1.0])
            one = 1.0 / float(table[0][2, 0])
            two = 1.0 / float(table[1][0, 0])
            rows = [
                jnp.where(order == 1, one * f, jnp.where(order == 2, two * s, r))
                for f, s, r in zip(first, second, rows)
            ]
        if l == 2:
            plus = [row[1:2] for row in below]
            minus = [row[2:3] for row in below]
            aa, bb = project(table, 2, a, plus), project(table, 2, b, minus)
            ab, ba = project(table, 2, a, minus), project(table, 2, b, plus)
            one = 1.0 / float(table[0][4, 2] - table[1][4, 0])
            two = 1.0 / float(table[0][0, 0] + table[1][0, 2])
            rows = [
                jnp.where(
                    order == 3,
                    one * (aa[m] - bb[m]),
                    jnp.where(order == 4, two * (ab[m] + ba[m]), rows[m]),
                )
                for m in range(5)
            ]
        for k, row in enumerate(rows):
            rot_ref[l * l + k] = row
        below = rows
    return length


STARTS = {"p1": 0, "n1": 768, "p2": 1536, "n2": 2176, "z": 2816}
LEFT_BLOCKS = 26


def left_rows(order, degree):
    if order == 0:
        return [(STARTS["z"] + 64 * degree, False)]
    m = (order + 1) // 2
    count = LMAX + 1 - m
    plus, minus = STARTS["p%d" % m], STARTS["n%d" % m]
    here = 64 * (degree - m)
    if order % 2:
        return [(plus + here, False), (minus + 64 * count + here, False)]
    return [(minus + here, False), (plus + 64 * count + here, True)]


def coefficient_row(k):
    return (k % TILES) * LANES + (k // TILES) * 64


GROUPS = [("z", (0, 1, 7)), ("y", (0,)), ("z", (2, 6)), ("y", (1, 3)), ("z", (3, 5, 4)), ("y", (2,))]


def group_tiles(axis):
    return range(0, Y_TILES) if axis == "z" else range(Y_TILES, TILES)


def group_needs(axis, offsets):
    return {
        (tile, oy, oz, side)
        for tile in group_tiles(axis)
        for oy in (range(Y_RING) if axis == "z" else offsets)
        for oz in (offsets if axis == "z" else range(Z_RING))
        for side in ("own", "other")
    }


PIECES = [((6, 5), 25, 12, 12), ((4, 3), 9, 8, 8), ((2, 1, 0), 0, 5, 4)]


def layer_kernel(
    nodes_ref,
    vector_ref,
    part_ref,
    slot_ref,
    target_ref,
    live_ref,
    zero_hbm,
    one_hbm,
    two_hbm,
    out_ref,
    table_ref,
    vectors_ref,
    zero_ref,
    one_ref,
    two_ref,
    rot_ref,
    pick_ref,
    states_ref,
    rows_ref,
    left_ref,
    sum_ref,
    parts_ref,
    landing_ref,
    send,
    recv,
    local,
    spread_sems,
    part_sems,
):
    edge = lax.axis_index("edge")
    chan = lax.axis_index("chan")
    edges = part_ref.shape[1]
    x = edge % 2
    z = (edge // 2) % Z_RING
    y = edge // (2 * Z_RING)

    def wrap(position, offset, size):
        return (position + (offset % size)) % size

    def device(dy, dz, side):
        return (wrap(y, dy, Y_RING) * Z_RING + wrap(z, dz, Z_RING)) * 2 + side

    reach = {link: device(dy, dz, x) for link, (dy, dz) in STEP.items() if link != "x"}
    reach["x"] = device(0, 0, 1 - x)
    barrier = pltpu.get_barrier_semaphore()
    for target in reach.values():
        pl.semaphore_signal(
            barrier, inc=1, device_id={"edge": target, "chan": chan}, device_id_type=MESH
        )
    for far in range(1, 4):
        pl.semaphore_signal(
            barrier,
            inc=1,
            device_id={"edge": edge, "chan": (chan + far) % 4},
            device_id_type=MESH,
        )
    loads = [
        pltpu.make_async_copy(src, dst, local.at[index])
        for index, (src, dst) in enumerate(
            ((one_hbm, one_ref), (two_hbm, two_ref), (zero_hbm, zero_ref))
        )
    ]
    for tile in range(TILES):
        low = nodes_ref[tile]
        high = nodes_ref[tile + TILES] if tile + TILES < COEFS else jnp.zeros_like(low)
        table_ref[y, z, x, tile] = jnp.concatenate([low, high], axis=1)
    vectors_ref[chan] = vector_ref[...]
    pl.semaphore_wait(barrier, 8)

    copies = []
    for index, (link, both, first, end, oy, oz) in enumerate(SENDS):
        view = table_ref.at[
            wrap(y, oy, Y_RING),
            wrap(z, oz, Z_RING),
            pl.ds(0, 2) if both else pl.ds(x, 1),
            pl.ds(first, end - first),
        ]
        copies.append(
            pltpu.make_async_remote_copy(
                src_ref=view,
                dst_ref=view,
                send_sem=send.at[index],
                recv_sem=recv.at[index],
                device_id={"edge": reach[link], "chan": chan},
                device_id_type=MESH,
            )
        )
    spread = [
        pltpu.make_async_remote_copy(
            src_ref=vector_ref,
            dst_ref=vectors_ref.at[chan],
            send_sem=spread_sems.at[far - 1],
            recv_sem=spread_sems.at[far + 2],
            device_id={"edge": edge, "chan": (chan + far) % 4},
            device_id_type=MESH,
        )
        for far in range(1, 4)
    ]

    scaling = []

    def begin_loads():
        for load in loads:
            load.start()

    def make_rotation():
        for copy in spread:
            copy.wait_recv()
        vectors = jnp.concatenate([vectors_ref[part] for part in range(4)], axis=1)
        length = wigner_into(rot_ref, vectors)
        alive = lax.broadcasted_iota(jnp.int32, (1, edges), 1) < live_ref[0]
        scaling.append(
            jnp.where(alive, 0.5 * (jnp.cos(length * (math.pi / CUTOFF)) + 1.0), 0.0)
        )

    def make_pick():
        source = part_ref[...] * 16 + slot_ref[...]
        row = lax.broadcasted_iota(jnp.int32, (32, edges), 0)
        for part in range(Y_RING * Z_RING):
            pick_ref[part // Z_RING, part % Z_RING] = jnp.where(
                source == row + 32 * part, 1.0, 0.0
            ).astype(jnp.bfloat16)

    def pick(axis, offsets, first, count, fresh):
        right, left = [], []
        for offset in offsets:
            if axis == "z":
                where = wrap(z, offset, Z_RING)
                right.append(pick_ref[:, where].reshape(128, edges))
            else:
                where = wrap(y, offset, Y_RING)
                right.append(pick_ref[where].reshape(256, edges))
            tiles = []
            for tile in range(first, first + count):
                if axis == "z":
                    part = table_ref[:, where, :, tile].reshape(128, LANES)
                else:
                    part = table_ref[where, :, :, tile].reshape(256, LANES)
                tiles.append(part.T)
            left.append(jnp.concatenate(tiles, axis=0) if count > 1 else tiles[0])
        left = jnp.concatenate(left, axis=1) if len(left) > 1 else left[0]
        right = jnp.concatenate(right, axis=0) if len(right) > 1 else right[0]
        picked = jnp.dot(left, right, preferred_element_type=jnp.float32).astype(jnp.bfloat16)
        rows = pl.ds(first * LANES, count * LANES)
        states_ref[rows, :] = picked if fresh else states_ref[rows, :] + picked

    have = {(tile, 0, 0, "own") for tile in range(TILES)}
    groups = list(GROUPS)
    seen = set()
    work = [begin_loads, make_pick, make_rotation]
    for kind, index in PROGRAM:
        if kind == "send":
            copies[index].start()
            if index == 3:
                for copy in spread:
                    copy.start()
            continue
        if index >= 10 and work:
            work.pop(0)()
        copies[index].wait_recv()
        have |= brought(index)
        while groups and group_needs(*groups[0]) <= have:
            axis, offsets = groups.pop(0)
            tiles = group_tiles(axis)
            for first in range(tiles[0], tiles[-1] + 1, 2):
                count = min(2, tiles[-1] + 1 - first)
                fresh = axis not in seen
                work.append(
                    lambda a=axis, o=offsets, f=first, c=count, n=fresh: pick(a, o, f, c, n)
                )
            seen.add(axis)
    for item in work:
        item()

    scale = jnp.broadcast_to(scaling[0], (16, edges))
    for degree in range(LMAX + 1):
        orders = 2 * min(degree, MMAX) + 1
        base = degree * degree

        def turn(chunk, carry, degree=degree, orders=orders, base=base):
            start = pl.multiple_of(chunk * 16, 16)
            totals = [None] * orders
            for k in range(2 * degree + 1):
                rows = pl.ds(coefficient_row(base + k) + start, 16)
                value = states_ref[rows, :].astype(jnp.float32)
                for order in range(orders):
                    factor = rot_ref[base + k, order : order + 1, :]
                    term = factor * value
                    totals[order] = term if k == 0 else totals[order] + term
            for order in range(orders):
                result = totals[order] * scale
                for first, negate in left_rows(order, degree):
                    rows_ref[pl.ds(first + start, 16), :] = (
                        -result if negate else result
                    ).astype(jnp.bfloat16)
            return carry

        lax.fori_loop(0, 4, turn, 0)

    def flip(block, carry):
        rows = pl.ds(pl.multiple_of(block * LANES, LANES), LANES)
        left_ref[block] = rows_ref[rows, :].T
        return carry

    lax.fori_loop(0, LEFT_BLOCKS, flip, 0)
    slot = lax.broadcasted_iota(jnp.int32, (16, edges), 0)
    chosen = jnp.where(slot == target_ref[...], 1.0, 0.0)

    def left(first, depth):
        blocks = [left_ref[first // LANES + i] for i in range(-(-depth // LANES))]
        return jnp.concatenate(blocks, axis=1)[:, :depth]

    def mix(order, degree, start, depth, right):
        mixed = jnp.dot(left(start, depth), right, preferred_element_type=jnp.float32)
        mixed = mixed.astype(jnp.bfloat16)
        back = jnp.concatenate(
            [
                (rot_ref[degree * degree + k, order : order + 1, :] * chosen).astype(jnp.bfloat16)
                for k in range(2 * degree + 1)
            ],
            axis=0,
        )
        rows = pl.ds(16 * degree * degree, 16 * (2 * degree + 1))
        value = jnp.dot(back, mixed, preferred_element_type=jnp.float32)
        sum_ref[rows, :] = value if order == 0 else sum_ref[rows, :] + value

    for load in loads:
        load.wait()
    outgoing = []
    base = 0
    for number, (degrees, first, lows, highs) in enumerate(PIECES):
        for degree in degrees:
            mix(0, degree, STARTS["z"], 448, zero_ref[:, degree].reshape(448, 256))
            if degree >= 1:
                right = one_ref[:, :, degree - 1].reshape(768, 256)
                mix(1, degree, STARTS["p1"], 768, right)
                mix(2, degree, STARTS["n1"], 768, right)
            if degree >= 2:
                right = two_ref[:, :, degree - 2].reshape(640, 256)
                mix(3, degree, STARTS["p2"], 640, right)
                mix(4, degree, STARTS["n2"], 640, right)
        for part in range(4):
            lanes = pl.ds(64 * part, 64)
            low = sum_ref[pl.ds(16 * first, 16 * lows), lanes]
            high = sum_ref[pl.ds(16 * (first + lows), 16 * highs), lanes]
            if highs < lows:
                high = jnp.concatenate(
                    [high, jnp.zeros((16 * (lows - highs), 64), jnp.float32)], axis=0
                )
            parts_ref[part, pl.ds(16 * base, 16 * lows)] = jnp.concatenate(
                [low, high], axis=1
            ).astype(jnp.bfloat16)
        piece = []
        for far in (2, 1, 3):
            target = (chan + far) % 4
            copy = pltpu.make_async_remote_copy(
                src_ref=parts_ref.at[target, pl.ds(16 * base, 16 * lows)],
                dst_ref=landing_ref.at[far - 1, pl.ds(16 * base, 16 * lows)],
                send_sem=part_sems.at[0, number, far - 1],
                recv_sem=part_sems.at[1, number, far - 1],
                device_id={"edge": edge, "chan": target},
                device_id_type=MESH,
            )
            copy.start()
            piece.append(copy)
        outgoing.append((base, piece))
        base += lows
    for (base, piece), (degrees, first, lows, highs) in zip(outgoing, PIECES):
        for copy in piece:
            copy.wait_recv()
        rows = pl.ds(16 * base, 16 * lows)
        total = parts_ref[chan, rows].astype(jnp.float32)
        for slot_number in range(3):
            total = total + landing_ref[slot_number, rows].astype(jnp.float32)
        total = total.astype(jnp.bfloat16)
        for step in range(lows):
            out_ref[first + step] = total[16 * step : 16 * step + 16, :64]
        for step in range(highs):
            out_ref[first + lows + step] = total[16 * step : 16 * step + 16, 64:]
    for copy in copies + spread:
        copy.wait_send()
    for _, piece in outgoing:
        for copy in piece:
            copy.wait_send()


def shards(
    node_states,
    edge_vectors,
    source_part,
    source_slot,
    target_slot,
    live_edges,
    weight_zero,
    weight_one,
    weight_two,
):
    edges = source_slot.shape[0]
    zero = weight_zero.transpose(0, 2, 1, 3)
    one = weight_one.transpose(0, 1, 3, 2, 4)
    two = weight_two.transpose(0, 1, 3, 2, 4)
    vmem = pl.BlockSpec(memory_space=pltpu.VMEM)
    hbm = pl.BlockSpec(memory_space=pl.ANY)
    result = pl.pallas_call(
        layer_kernel,
        name="layer",
        out_shape=jax.ShapeDtypeStruct((COEFS, 16, 64), jnp.bfloat16),
        in_specs=[vmem] * 5 + [pl.BlockSpec(memory_space=pltpu.SMEM), hbm, hbm, hbm],
        out_specs=vmem,
        scratch_shapes=[
            pltpu.VMEM((Y_RING, Z_RING, 2, TILES, 16, LANES), jnp.bfloat16),
            pltpu.VMEM((4, 3, LANES), jnp.float32),
            pltpu.VMEM(zero.shape, jnp.bfloat16),
            pltpu.VMEM(one.shape, jnp.bfloat16),
            pltpu.VMEM(two.shape, jnp.bfloat16),
            pltpu.VMEM((COEFS, 8, edges), jnp.float32),
            pltpu.VMEM((Y_RING, Z_RING, 32, edges), jnp.bfloat16),
            pltpu.VMEM((TILES * LANES, edges), jnp.bfloat16),
            pltpu.VMEM((LEFT_BLOCKS * LANES, edges), jnp.bfloat16),
            pltpu.VMEM((LEFT_BLOCKS, edges, LANES), jnp.bfloat16),
            pltpu.VMEM((16 * COEFS, 256), jnp.float32),
            pltpu.VMEM((4, 400, LANES), jnp.bfloat16),
            pltpu.VMEM((3, 400, LANES), jnp.bfloat16),
            pltpu.SemaphoreType.DMA((len(SENDS),)),
            pltpu.SemaphoreType.DMA((len(SENDS),)),
            pltpu.SemaphoreType.DMA((3,)),
            pltpu.SemaphoreType.DMA((6,)),
            pltpu.SemaphoreType.DMA((2, 3, 3)),
        ],
        compiler_params=pltpu.CompilerParams(
            collective_id=0, has_side_effects=True, vmem_limit_bytes=60 << 20
        ),
    )(
        node_states.transpose(1, 0, 2),
        edge_vectors,
        source_part.reshape(1, edges),
        source_slot.reshape(1, edges),
        target_slot.reshape(1, edges),
        live_edges,
        zero,
        one,
        two,
    )
    return result.transpose(1, 0, 2)


def solution(mesh):
    in_specs = (
        P("edge", None, "chan"),
        P(None, ("edge", "chan")),
        P("edge", None),
        P("edge"),
        P("edge"),
        P("edge"),
        P(None, "chan", None, None),
        P(None, None, "chan", None, None),
        P(None, None, "chan", None, None),
    )
    out_specs = P("edge", None, "chan")
    return jax.shard_map(shards, mesh=mesh, in_specs=in_specs, out_specs=out_specs, check_vma=False)
```

```python
import math

import jax
import jax.numpy as jnp
import numpy as np
from jax import lax
from jax.experimental import pallas as pl
from jax.experimental.pallas import tpu as pltpu
from jax.sharding import PartitionSpec as P

LMAX = 6
MMAX = 2
COEFS = (LMAX + 1) ** 2
CUTOFF = 6.0
LANES = 128
TILES = 25
MESH = pl.DeviceIdType.MESH

Y_RING, Z_RING = 4, 8
STEP = {"y+": (1, 0), "y-": (-1, 0), "z+": (0, 1), "z-": (0, -1), "x": (0, 0)}
COLOURS = {
    "py": ("y", True, ((0, 3), (3, 6))),
    "sy": ("y", False, ((6, 8), (8, 10))),
    "pz": ("z", True, ((10, 15), (15, 19))),
    "sz": ("z", False, ((19, 22), (22, 25))),
}
Y_TILES = 10
LATENCY, BYTES_PER_US, BLOCK_TILE, SLACK = 2.8, 46e3, 4096, 3.0


def schedule():
    free = {link: 0.0 for link in STEP}
    waiting = {link: [] for link in STEP}
    events, sends, begun, landed, passed = [], [], [], [], set()
    count = 0

    def put(link, time, rank, colour, half, oy, oz, sides):
        nonlocal count
        waiting[link].append((time, -rank, count, colour, half, oy, oz, sides))
        count += 1

    def follow(time, colour, half, oy, oz, via, brings):
        axis_first, paired, _ = COLOURS[colour]
        sides = "both" if paired else "own"
        if via == "x" and not paired:
            return
        if via not in ("", "x") and paired and brings == "own":
            return
        if not via or via == "x":
            sides = "own" if not via else "other"
            via = ""
        if not paired:
            put("x", time, 0, colour, half, oy, oz, "own")
        second = "z" if axis_first == "y" else "y"
        offset = {"y": oy, "z": oz}
        limit = {"y": Y_RING // 2, "z": Z_RING // 2}

        def along(axis, rank):
            moved = offset[axis]
            for sign, mine in (("+", 0), ("-", 1)):
                hops = abs(moved) + 1
                if (moved != 0 and via != axis + sign) or hops > limit[axis]:
                    continue
                taken = (mine,) if hops == limit[axis] else half
                taken = tuple(h for h in taken if h in half)
                if taken:
                    put(
                        axis + sign,
                        time,
                        rank + limit[axis] - hops + (0 if paired else 1),
                        colour,
                        taken,
                        oy,
                        oz,
                        sides,
                    )

        if offset[second] == 0:
            along(axis_first, 10)
        along(second, 0)

    for colour, (_, paired, _) in COLOURS.items():
        if paired:
            put("x", 0.0, 20, colour, (0, 1), 0, 0, "own")
        follow(0.0, colour, (0, 1), 0, 0, "", "own")
    while events or any(waiting.values()):
        ready = [
            (max(free[link], min(item[0] for item in items)), link)
            for link, items in waiting.items()
            if items
        ]
        begin = min(ready) if ready else None
        if events and (begin is None or min(events)[0] <= begin[0]):
            event = min(events)
            events.remove(event)
            time, number, colour, half, oy, oz, via, brings = event
            before = count
            follow(time, colour, half, oy, oz, via, brings)
            if count > before or brings == "own" and COLOURS[colour][1]:
                passed.add(number)
            continue
        time, link = begin
        item = min(
            (item for item in waiting[link] if item[0] <= time),
            key=lambda it: (it[1], it[0], it[2]),
        )
        waiting[link].remove(item)
        known, _, _, colour, half, oy, oz, sides = item
        halves = COLOURS[colour][2]
        first, end = halves[half[0]][0], halves[half[-1]][1]
        blocks = 2 if sides == "both" else 1
        free[link] = time + (end - first) * blocks * BLOCK_TILE / BYTES_PER_US
        earlier = [b for b, s in zip(begun, sends) if s[0] == link]
        dy, dz = STEP[link]
        sends.append((link, sides, first, end, oy, oz))
        begun.append(max([known] + earlier[-1:]))
        landed.append(free[link] + LATENCY)
        events.append((landed[-1], len(sends) - 1, colour, half, oy - dy, oz - dz, link, sides))
    steps = [(time, 1, index, "send") for index, time in enumerate(begun)]
    steps += [
        (time + (0.0 if index in passed else SLACK), 0, index, "wait")
        for index, time in enumerate(landed)
    ]
    return sends, [(kind, index) for _, _, index, kind in sorted(steps)]


SENDS, PROGRAM = schedule()


def brought(index):
    link, sides, first, end, oy, oz = SENDS[index]
    dy, dz = STEP[link]
    if link == "x":
        sides = "other"
    sides = ("own", "other") if sides == "both" else (sides,)
    return {
        (tile, (oy - dy) % Y_RING, (oz - dz) % Z_RING, side)
        for tile in range(first, end)
        for side in sides
    }


def harmonics_at(points, degree_top):
    x, y, z = points
    rows = {}
    real, imag = [np.ones_like(x)], [np.zeros_like(x)]
    for m in range(1, degree_top + 1):
        real.append(x * real[m - 1] - y * imag[m - 1])
        imag.append(x * imag[m - 1] + y * real[m - 1])
    for m in range(degree_top + 1):
        start = (-1.0) ** m * math.prod(range(2 * m - 1, 0, -2))
        legendre = {m: np.full_like(z, start), m + 1: z * ((2 * m + 1) * start)}
        for l in range(m + 2, degree_top + 1):
            legendre[l] = (
                (2 * l - 1) * z * legendre[l - 1] - (l + m - 1) * legendre[l - 2]
            ) / (l - m)
        for l in range(m, degree_top + 1):
            factor = math.sqrt(
                (2 * l + 1) / (4 * math.pi) * math.factorial(l - m) / math.factorial(l + m)
            )
            if m == 0:
                rows[l, 0] = factor * legendre[l]
            else:
                rows[l, m] = math.sqrt(2.0) * factor * legendre[l] * real[m]
                rows[l, -m] = math.sqrt(2.0) * factor * legendre[l] * imag[m]
    return np.stack([rows[l, m] for l in range(degree_top + 1) for m in range(-l, l + 1)])


def raising_tables():
    count = 4 * (LMAX + 2) ** 2
    at = np.arange(count) + 0.5
    height = 1.0 - 2.0 * at / count
    radius = np.sqrt(1.0 - height * height)
    angle = math.pi * (3.0 - math.sqrt(5.0)) * at
    points = np.stack([radius * np.cos(angle), radius * np.sin(angle), height])
    basis = harmonics_at(points, LMAX)
    inverse = np.linalg.pinv(basis.T)
    tables = {}
    for l in range(1, LMAX + 1):
        below = basis[(l - 1) ** 2 : l * l]
        tables[l] = [
            np.where(np.abs(part) < 1e-9, 0.0, part)
            for part in (
                (inverse @ (points[c] * below).T)[l * l : (l + 1) ** 2] for c in range(3)
            )
        ]
    return tables


RAISE = raising_tables()


def project(table, degree, weights, rows):
    results = []
    for m in range(2 * degree + 1):
        total = None
        for axis in range(3):
            for n in range(2 * degree - 1):
                value = float(table[axis][m, n])
                if value != 0.0:
                    term = (value * weights[axis]) * rows[n]
                    total = term if total is None else total + term
        results.append(total)
    return results


def wigner_into(rot_ref, vectors):
    x, y, z = vectors[0:1], vectors[1:2], vectors[2:3]
    length = jnp.sqrt(x * x + y * y + z * z)
    u = [x / length, y / length, z / length]
    pick = jnp.where(jnp.abs(u[0]) < 0.6, 1.0, 0.0)
    other = 1.0 - pick
    a = [-u[2] * other, u[2] * pick, u[0] * other - u[1] * pick]
    norm = jnp.sqrt(a[0] * a[0] + a[1] * a[1] + a[2] * a[2])
    a = [part / norm for part in a]
    b = [
        u[1] * a[2] - u[2] * a[1],
        u[2] * a[0] - u[0] * a[2],
        u[0] * a[1] - u[1] * a[0],
    ]
    shape = (8, x.shape[1])
    order = lax.broadcasted_iota(jnp.int32, shape, 0)
    wide = [jnp.broadcast_to(part, shape) for part in u]
    below = [jnp.where(order == 0, 1.0, 0.0)]
    rot_ref[0] = below[0]
    for l in range(1, LMAX + 1):
        table = RAISE[l]
        inverse = [1.0 / float(table[2][m + l, m + l - 1]) if m < l else 0.0 for m in range(3)]
        scale = jnp.where(
            order == 0, inverse[0], jnp.where(order <= 2, inverse[1], inverse[2])
        )
        rows = project(table, l, [part * scale for part in wide], below)
        rows = [jnp.zeros(shape, jnp.float32) if row is None else row for row in rows]
        if l == 1:
            first = project(table, 1, a, [1.0])
            second = project(table, 1, b, [1.0])
            one = 1.0 / float(table[0][2, 0])
            two = 1.0 / float(table[1][0, 0])
            rows = [
                jnp.where(order == 1, one * f, jnp.where(order == 2, two * s, r))
                for f, s, r in zip(first, second, rows)
            ]
        if l == 2:
            plus = [row[1:2] for row in below]
            minus = [row[2:3] for row in below]
            aa, bb = project(table, 2, a, plus), project(table, 2, b, minus)
            ab, ba = project(table, 2, a, minus), project(table, 2, b, plus)
            one = 1.0 / float(table[0][4, 2] - table[1][4, 0])
            two = 1.0 / float(table[0][0, 0] + table[1][0, 2])
            rows = [
                jnp.where(
                    order == 3,
                    one * (aa[m] - bb[m]),
                    jnp.where(order == 4, two * (ab[m] + ba[m]), rows[m]),
                )
                for m in range(5)
            ]
        for k, row in enumerate(rows):
            rot_ref[l * l + k] = row
        below = rows
    return length


STARTS = {"p1": 0, "n1": 768, "p2": 1536, "n2": 2176, "z": 2816}
LEFT_BLOCKS = 26


def left_rows(order, degree):
    if order == 0:
        return [(STARTS["z"] + 64 * degree, False)]
    m = (order + 1) // 2
    count = LMAX + 1 - m
    plus, minus = STARTS["p%d" % m], STARTS["n%d" % m]
    here = 64 * (degree - m)
    if order % 2:
        return [(plus + here, False), (minus + 64 * count + here, False)]
    return [(minus + here, False), (plus + 64 * count + here, True)]


def coefficient_row(k):
    return (k % TILES) * LANES + (k // TILES) * 64


GROUPS = [("z", (0, 1, 7)), ("y", (0,)), ("z", (2, 6)), ("y", (1, 3)), ("z", (3, 5, 4)), ("y", (2,))]


def group_tiles(axis):
    return range(0, Y_TILES) if axis == "z" else range(Y_TILES, TILES)


def group_needs(axis, offsets):
    return {
        (tile, oy, oz, side)
        for tile in group_tiles(axis)
        for oy in (range(Y_RING) if axis == "z" else offsets)
        for oz in (offsets if axis == "z" else range(Z_RING))
        for side in ("own", "other")
    }


PIECES = [
    ((6,), 36, 7, 6),
    ((5,), 25, 6, 5),
    ((4,), 16, 5, 4),
    ((3,), 9, 4, 3),
    ((0, 1, 2), 0, 5, 4),
]
PART_ROWS = 16 * sum(piece[2] for piece in PIECES)


def layer_kernel(
    nodes_hbm,
    vector_hbm,
    part_hbm,
    slot_hbm,
    target_hbm,
    live_ref,
    zero_hbm,
    one_hbm,
    two_hbm,
    out_ref,
    nodes_ref,
    vector_ref,
    part_ref,
    slot_ref,
    target_ref,
    table_ref,
    vectors_ref,
    zero_ref,
    one_ref,
    two_ref,
    rot_ref,
    pick_ref,
    states_ref,
    rows_ref,
    left_ref,
    mixed_ref,
    parts_ref,
    landing_ref,
    send,
    recv,
    local,
    spread_sems,
    part_sems,
):
    edge = lax.axis_index("edge")
    chan = lax.axis_index("chan")
    edges = part_ref.shape[1]
    reads = [
        pltpu.make_async_copy(src, dst, local.at[3 + index])
        for index, (src, dst) in enumerate(
            (
                (nodes_hbm, nodes_ref),
                (vector_hbm, vector_ref),
                (part_hbm, part_ref),
                (slot_hbm, slot_ref),
                (target_hbm, target_ref),
            )
        )
    ]
    for read in reads:
        read.start()
    x = edge % 2
    z = (edge // 2) % Z_RING
    y = edge // (2 * Z_RING)

    def wrap(position, offset, size):
        return (position + (offset % size)) % size

    def device(dy, dz, side):
        return (wrap(y, dy, Y_RING) * Z_RING + wrap(z, dz, Z_RING)) * 2 + side

    reach = {link: device(dy, dz, x) for link, (dy, dz) in STEP.items() if link != "x"}
    reach["x"] = device(0, 0, 1 - x)
    barrier = pltpu.get_barrier_semaphore()
    for target in reach.values():
        pl.semaphore_signal(
            barrier, inc=1, device_id={"edge": target, "chan": chan}, device_id_type=MESH
        )
    for far in range(1, 4):
        pl.semaphore_signal(
            barrier,
            inc=1,
            device_id={"edge": edge, "chan": (chan + far) % 4},
            device_id_type=MESH,
        )
    loads = [
        pltpu.make_async_copy(src, dst, local.at[index])
        for index, (src, dst) in enumerate(
            ((one_hbm, one_ref), (two_hbm, two_ref), (zero_hbm, zero_ref))
        )
    ]
    for read in reads:
        read.wait()
    for tile in range(TILES):
        low = nodes_ref[tile]
        high = nodes_ref[tile + TILES] if tile + TILES < COEFS else jnp.zeros_like(low)
        table_ref[y, z, x, tile] = jnp.concatenate([low, high], axis=1)
    vectors_ref[chan] = vector_ref[...]
    pl.semaphore_wait(barrier, 8)

    copies = []
    span = {"both": pl.ds(0, 2), "own": pl.ds(x, 1), "other": pl.ds(1 - x, 1)}
    for index, (link, sides, first, end, oy, oz) in enumerate(SENDS):
        view = table_ref.at[
            wrap(y, oy, Y_RING),
            wrap(z, oz, Z_RING),
            span[sides],
            pl.ds(first, end - first),
        ]
        copies.append(
            pltpu.make_async_remote_copy(
                src_ref=view,
                dst_ref=view,
                send_sem=send.at[index],
                recv_sem=recv.at[index],
                device_id={"edge": reach[link], "chan": chan},
                device_id_type=MESH,
            )
        )
    spread = [
        pltpu.make_async_remote_copy(
            src_ref=vector_ref,
            dst_ref=vectors_ref.at[chan],
            send_sem=spread_sems.at[far - 1],
            recv_sem=spread_sems.at[far + 2],
            device_id={"edge": edge, "chan": (chan + far) % 4},
            device_id_type=MESH,
        )
        for far in range(1, 4)
    ]

    scaling = []

    def begin_loads():
        for load in loads:
            load.start()

    def make_rotation():
        for copy in spread:
            copy.wait_recv()
        vectors = jnp.concatenate([vectors_ref[part] for part in range(4)], axis=1)
        length = wigner_into(rot_ref, vectors)
        alive = lax.broadcasted_iota(jnp.int32, (1, edges), 1) < live_ref[0]
        scaling.append(
            jnp.where(alive, 0.5 * (jnp.cos(length * (math.pi / CUTOFF)) + 1.0), 0.0)
        )

    def make_pick():
        source = part_ref[...] * 16 + slot_ref[...]
        row = lax.broadcasted_iota(jnp.int32, (32, edges), 0)
        for part in range(Y_RING * Z_RING):
            pick_ref[part // Z_RING, part % Z_RING] = jnp.where(
                source == row + 32 * part, 1.0, 0.0
            ).astype(jnp.bfloat16)

    def pick(axis, offsets, first, count, fresh):
        right, left = [], []
        for offset in offsets:
            if axis == "z":
                where = wrap(z, offset, Z_RING)
                right.append(pick_ref[:, where].reshape(128, edges))
            else:
                where = wrap(y, offset, Y_RING)
                right.append(pick_ref[where].reshape(256, edges))
            tiles = []
            for tile in range(first, first + count):
                if axis == "z":
                    part = table_ref[:, where, :, tile].reshape(128, LANES)
                else:
                    part = table_ref[where, :, :, tile].reshape(256, LANES)
                tiles.append(part.T)
            left.append(jnp.concatenate(tiles, axis=0) if count > 1 else tiles[0])
        left = jnp.concatenate(left, axis=1) if len(left) > 1 else left[0]
        right = jnp.concatenate(right, axis=0) if len(right) > 1 else right[0]
        picked = jnp.dot(left, right, preferred_element_type=jnp.float32).astype(jnp.bfloat16)
        rows = pl.ds(first * LANES, count * LANES)
        states_ref[rows, :] = picked if fresh else states_ref[rows, :] + picked

    have = {(tile, 0, 0, "own") for tile in range(TILES)}
    groups = list(GROUPS)
    seen = set()
    work = [begin_loads, make_pick, make_rotation]
    for kind, index in PROGRAM:
        if kind == "send":
            copies[index].start()
            if index == 3:
                for copy in spread:
                    copy.start()
            continue
        if index >= 10 and work:
            work.pop(0)()
        copies[index].wait_recv()
        have |= brought(index)
        while groups and group_needs(*groups[0]) <= have:
            axis, offsets = groups.pop(0)
            tiles = group_tiles(axis)
            for first in range(tiles[0], tiles[-1] + 1, 2):
                count = min(2, tiles[-1] + 1 - first)
                fresh = axis not in seen
                work.append(
                    lambda a=axis, o=offsets, f=first, c=count, n=fresh: pick(a, o, f, c, n)
                )
            seen.add(axis)
    for item in work:
        item()

    scale = jnp.broadcast_to(scaling[0], (16, edges))
    for degree in range(LMAX + 1):
        orders = 2 * min(degree, MMAX) + 1
        base = degree * degree

        def turn(chunk, carry, degree=degree, orders=orders, base=base):
            start = pl.multiple_of(chunk * 16, 16)
            totals = [None] * orders
            for k in range(2 * degree + 1):
                rows = pl.ds(coefficient_row(base + k) + start, 16)
                value = states_ref[rows, :].astype(jnp.float32)
                for order in range(orders):
                    factor = rot_ref[base + k, order : order + 1, :]
                    term = factor * value
                    totals[order] = term if k == 0 else totals[order] + term
            for order in range(orders):
                result = totals[order] * scale
                for first, negate in left_rows(order, degree):
                    rows_ref[pl.ds(first + start, 16), :] = (
                        -result if negate else result
                    ).astype(jnp.bfloat16)
            return carry

        lax.fori_loop(0, 4, turn, 0)

    def flip(block, carry):
        rows = pl.ds(pl.multiple_of(block * LANES, LANES), LANES)
        left_ref[block] = rows_ref[rows, :].T
        return carry

    lax.fori_loop(0, LEFT_BLOCKS, flip, 0)
    slot = lax.broadcasted_iota(jnp.int32, (16, edges), 0)
    chosen = jnp.where(slot == target_ref[...], 1.0, 0.0)

    def left(first, depth):
        blocks = [left_ref[first // LANES + i] for i in range(-(-depth // LANES))]
        return jnp.concatenate(blocks, axis=1)[:, :depth]

    def mix(turn_of, order, start, depth, right):
        mixed = jnp.dot(left(start, depth), right, preferred_element_type=jnp.float32)
        mixed_ref[turn_of, order] = mixed.astype(jnp.bfloat16)

    def degree_sum(degree, turn_of):
        mix(turn_of, 0, STARTS["z"], 448, zero_ref[:, degree].reshape(448, 256))
        if degree >= 1:
            right = one_ref[:, :, degree - 1].reshape(768, 256)
            mix(turn_of, 1, STARTS["p1"], 768, right)
            mix(turn_of, 2, STARTS["n1"], 768, right)
        if degree >= 2:
            right = two_ref[:, :, degree - 2].reshape(640, 256)
            mix(turn_of, 3, STARTS["p2"], 640, right)
            mix(turn_of, 4, STARTS["n2"], 640, right)
        orders = 2 * min(degree, MMAX) + 1
        back = [
            jnp.concatenate(
                [
                    (rot_ref[degree * degree + k, order : order + 1, :] * chosen).astype(
                        jnp.bfloat16
                    )
                    for k in range(2 * degree + 1)
                ],
                axis=0,
            )
            for order in range(orders)
        ]
        back = jnp.concatenate(back, axis=1) if orders > 1 else back[0]
        mixed = mixed_ref[turn_of, 0:orders].reshape(orders * edges, 256)
        return jnp.dot(back, mixed, preferred_element_type=jnp.float32)

    for load in loads:
        load.wait()
    outgoing = []
    base = 0
    for number, (degrees, first, lows, highs) in enumerate(PIECES):
        sums = [degree_sum(degree, degree % 2) for degree in degrees]
        sums = jnp.concatenate(sums, axis=0) if len(sums) > 1 else sums[0]
        if highs < lows:
            sums = jnp.concatenate([sums, jnp.zeros((16, 256), jnp.float32)], axis=0)
        for part in range(4):
            lanes = slice(64 * part, 64 * part + 64)
            parts_ref[part, pl.ds(16 * base, 16 * lows)] = jnp.concatenate(
                [sums[: 16 * lows, lanes], sums[16 * lows :, lanes]], axis=1
            ).astype(jnp.bfloat16)
        piece = []
        for far in (2, 1, 3):
            target = (chan + far) % 4
            copy = pltpu.make_async_remote_copy(
                src_ref=parts_ref.at[target, pl.ds(16 * base, 16 * lows)],
                dst_ref=landing_ref.at[far - 1, pl.ds(16 * base, 16 * lows)],
                send_sem=part_sems.at[0, number, far - 1],
                recv_sem=part_sems.at[1, number, far - 1],
                device_id={"edge": edge, "chan": target},
                device_id_type=MESH,
            )
            copy.start()
            piece.append(copy)
        outgoing.append((base, piece))
        base += lows
    for (base, piece), (degrees, first, lows, highs) in zip(outgoing, PIECES):
        for copy in piece:
            copy.wait_recv()
        rows = pl.ds(16 * base, 16 * lows)
        total = parts_ref[chan, rows].astype(jnp.float32)
        for slot_number in range(3):
            total = total + landing_ref[slot_number, rows].astype(jnp.float32)
        total = total.astype(jnp.bfloat16)
        for step in range(lows):
            out_ref[first + step] = total[16 * step : 16 * step + 16, :64]
        for step in range(highs):
            out_ref[first + lows + step] = total[16 * step : 16 * step + 16, 64:]
    for copy in copies + spread:
        copy.wait_send()
    for _, piece in outgoing:
        for copy in piece:
            copy.wait_send()


def shards(
    node_states,
    edge_vectors,
    source_part,
    source_slot,
    target_slot,
    live_edges,
    weight_zero,
    weight_one,
    weight_two,
):
    edges = source_slot.shape[0]
    zero = weight_zero.transpose(0, 2, 1, 3)
    one = weight_one.transpose(0, 1, 3, 2, 4)
    two = weight_two.transpose(0, 1, 3, 2, 4)
    vmem = pl.BlockSpec(memory_space=pltpu.VMEM)
    hbm = pl.BlockSpec(memory_space=pl.ANY)
    result = pl.pallas_call(
        layer_kernel,
        name="layer",
        out_shape=jax.ShapeDtypeStruct((COEFS, 16, 64), jnp.bfloat16),
        in_specs=[hbm] * 5 + [pl.BlockSpec(memory_space=pltpu.SMEM), hbm, hbm, hbm],
        out_specs=vmem,
        scratch_shapes=[
            pltpu.VMEM((COEFS, 16, 64), jnp.bfloat16),
            pltpu.VMEM((3, LANES), jnp.float32),
            pltpu.VMEM((1, edges), jnp.int32),
            pltpu.VMEM((1, edges), jnp.int32),
            pltpu.VMEM((1, edges), jnp.int32),
            pltpu.VMEM((Y_RING, Z_RING, 2, TILES, 16, LANES), jnp.bfloat16),
            pltpu.VMEM((4, 3, LANES), jnp.float32),
            pltpu.VMEM(zero.shape, jnp.bfloat16),
            pltpu.VMEM(one.shape, jnp.bfloat16),
            pltpu.VMEM(two.shape, jnp.bfloat16),
            pltpu.VMEM((COEFS, 8, edges), jnp.float32),
            pltpu.VMEM((Y_RING, Z_RING, 32, edges), jnp.bfloat16),
            pltpu.VMEM((TILES * LANES, edges), jnp.bfloat16),
            pltpu.VMEM((LEFT_BLOCKS * LANES, edges), jnp.bfloat16),
            pltpu.VMEM((LEFT_BLOCKS, edges, LANES), jnp.bfloat16),
            pltpu.VMEM((2, 5, edges, 256), jnp.bfloat16),
            pltpu.VMEM((4, PART_ROWS, LANES), jnp.bfloat16),
            pltpu.VMEM((3, PART_ROWS, LANES), jnp.bfloat16),
            pltpu.SemaphoreType.DMA((len(SENDS),)),
            pltpu.SemaphoreType.DMA((len(SENDS),)),
            pltpu.SemaphoreType.DMA((8,)),
            pltpu.SemaphoreType.DMA((6,)),
            pltpu.SemaphoreType.DMA((2, len(PIECES), 3)),
        ],
        compiler_params=pltpu.CompilerParams(
            collective_id=0, has_side_effects=True, vmem_limit_bytes=60 << 20
        ),
    )(
        node_states.transpose(1, 0, 2),
        edge_vectors,
        source_part.reshape(1, edges),
        source_slot.reshape(1, edges),
        target_slot.reshape(1, edges),
        live_edges,
        zero,
        one,
        two,
    )
    return result.transpose(1, 0, 2)


def solution(mesh):
    in_specs = (
        P("edge", None, "chan"),
        P(None, ("edge", "chan")),
        P("edge", None),
        P("edge"),
        P("edge"),
        P("edge"),
        P(None, "chan", None, None),
        P(None, None, "chan", None, None),
        P(None, None, "chan", None, None),
    )
    out_specs = P("edge", None, "chan")
    return jax.shard_map(shards, mesh=mesh, in_specs=in_specs, out_specs=out_specs, check_vma=False)
```

```python
import math

import jax
import jax.numpy as jnp
import numpy as np
from jax import lax
from jax.experimental import pallas as pl
from jax.experimental.pallas import tpu as pltpu
from jax.sharding import PartitionSpec as P

LMAX = 6
MMAX = 2
COEFS = (LMAX + 1) ** 2
CUTOFF = 6.0
LANES = 128
TILES = 25
MESH = pl.DeviceIdType.MESH

Y_RING, Z_RING = 4, 8
STEP = {"y+": (1, 0), "y-": (-1, 0), "z+": (0, 1), "z-": (0, -1), "x": (0, 0)}
COLOURS = {
    "py": ("y", True, ((0, 3), (3, 6))),
    "sy": ("y", False, ((6, 8), (8, 10))),
    "pz": ("z", True, ((10, 15), (15, 19))),
    "sz": ("z", False, ((19, 22), (22, 25))),
}
Y_TILES = 10
LATENCY, BYTES_PER_US, BLOCK_TILE, SLACK = 2.8, 46e3, 4096, 1.0


def schedule():
    free = {link: 0.0 for link in STEP}
    waiting = {link: [] for link in STEP}
    events, sends, begun, landed, passed = [], [], [], [], set()
    count = 0

    def put(link, time, rank, colour, half, oy, oz, sides):
        nonlocal count
        waiting[link].append((time, -rank, count, colour, half, oy, oz, sides))
        count += 1

    def follow(time, colour, half, oy, oz, via, brings):
        axis_first, paired, _ = COLOURS[colour]
        sides = "both" if paired else "own"
        if via == "x" and not paired:
            return
        if via not in ("", "x") and paired and brings == "own":
            return
        if not via or via == "x":
            sides = "own" if not via else "other"
            via = ""
        if not paired:
            put("x", time, 0, colour, half, oy, oz, "own")
        second = "z" if axis_first == "y" else "y"
        offset = {"y": oy, "z": oz}
        limit = {"y": Y_RING // 2, "z": Z_RING // 2}

        def along(axis, rank):
            moved = offset[axis]
            for sign, mine in (("+", 0), ("-", 1)):
                hops = abs(moved) + 1
                if (moved != 0 and via != axis + sign) or hops > limit[axis]:
                    continue
                taken = (mine,) if hops == limit[axis] else half
                taken = tuple(h for h in taken if h in half)
                if taken:
                    put(
                        axis + sign,
                        time,
                        rank + limit[axis] - hops + (0 if paired else 1),
                        colour,
                        taken,
                        oy,
                        oz,
                        sides,
                    )

        if offset[second] == 0:
            along(axis_first, 10)
        along(second, 0)

    for colour, (_, paired, _) in COLOURS.items():
        if paired:
            put("x", 0.0, 20, colour, (0, 1), 0, 0, "own")
        follow(0.0, colour, (0, 1), 0, 0, "", "own")
    while events or any(waiting.values()):
        ready = [
            (max(free[link], min(item[0] for item in items)), link)
            for link, items in waiting.items()
            if items
        ]
        begin = min(ready) if ready else None
        if events and (begin is None or min(events)[0] <= begin[0]):
            event = min(events)
            events.remove(event)
            time, number, colour, half, oy, oz, via, brings = event
            before = count
            follow(time, colour, half, oy, oz, via, brings)
            if count > before or brings == "own" and COLOURS[colour][1]:
                passed.add(number)
            continue
        time, link = begin
        item = min(
            (item for item in waiting[link] if item[0] <= time),
            key=lambda it: (it[1], it[0], it[2]),
        )
        waiting[link].remove(item)
        known, _, _, colour, half, oy, oz, sides = item
        halves = COLOURS[colour][2]
        first, end = halves[half[0]][0], halves[half[-1]][1]
        blocks = 2 if sides == "both" else 1
        free[link] = time + (end - first) * blocks * BLOCK_TILE / BYTES_PER_US
        earlier = [b for b, s in zip(begun, sends) if s[0] == link]
        dy, dz = STEP[link]
        sends.append((link, sides, first, end, oy, oz))
        begun.append(max([known] + earlier[-1:]))
        landed.append(free[link] + LATENCY)
        events.append((landed[-1], len(sends) - 1, colour, half, oy - dy, oz - dz, link, sides))
    steps = [(time, 1, index, "send") for index, time in enumerate(begun)]
    steps += [
        (time + (0.0 if index in passed else SLACK), 0, index, "wait")
        for index, time in enumerate(landed)
    ]
    return sends, [(kind, index) for _, _, index, kind in sorted(steps)]


SENDS, PROGRAM = schedule()


def brought(index):
    link, sides, first, end, oy, oz = SENDS[index]
    dy, dz = STEP[link]
    if link == "x":
        sides = "other"
    sides = ("own", "other") if sides == "both" else (sides,)
    return {
        (tile, (oy - dy) % Y_RING, (oz - dz) % Z_RING, side)
        for tile in range(first, end)
        for side in sides
    }


def harmonics_at(points, degree_top):
    x, y, z = points
    rows = {}
    real, imag = [np.ones_like(x)], [np.zeros_like(x)]
    for m in range(1, degree_top + 1):
        real.append(x * real[m - 1] - y * imag[m - 1])
        imag.append(x * imag[m - 1] + y * real[m - 1])
    for m in range(degree_top + 1):
        start = (-1.0) ** m * math.prod(range(2 * m - 1, 0, -2))
        legendre = {m: np.full_like(z, start), m + 1: z * ((2 * m + 1) * start)}
        for l in range(m + 2, degree_top + 1):
            legendre[l] = (
                (2 * l - 1) * z * legendre[l - 1] - (l + m - 1) * legendre[l - 2]
            ) / (l - m)
        for l in range(m, degree_top + 1):
            factor = math.sqrt(
                (2 * l + 1) / (4 * math.pi) * math.factorial(l - m) / math.factorial(l + m)
            )
            if m == 0:
                rows[l, 0] = factor * legendre[l]
            else:
                rows[l, m] = math.sqrt(2.0) * factor * legendre[l] * real[m]
                rows[l, -m] = math.sqrt(2.0) * factor * legendre[l] * imag[m]
    return np.stack([rows[l, m] for l in range(degree_top + 1) for m in range(-l, l + 1)])


def raising_tables():
    count = 4 * (LMAX + 2) ** 2
    at = np.arange(count) + 0.5
    height = 1.0 - 2.0 * at / count
    radius = np.sqrt(1.0 - height * height)
    angle = math.pi * (3.0 - math.sqrt(5.0)) * at
    points = np.stack([radius * np.cos(angle), radius * np.sin(angle), height])
    basis = harmonics_at(points, LMAX)
    inverse = np.linalg.pinv(basis.T)
    tables = {}
    for l in range(1, LMAX + 1):
        below = basis[(l - 1) ** 2 : l * l]
        tables[l] = [
            np.where(np.abs(part) < 1e-9, 0.0, part)
            for part in (
                (inverse @ (points[c] * below).T)[l * l : (l + 1) ** 2] for c in range(3)
            )
        ]
    return tables


RAISE = raising_tables()


def project(table, degree, weights, rows):
    results = []
    for m in range(2 * degree + 1):
        total = None
        for axis in range(3):
            for n in range(2 * degree - 1):
                value = float(table[axis][m, n])
                if value != 0.0:
                    term = (value * weights[axis]) * rows[n]
                    total = term if total is None else total + term
        results.append(total)
    return results


def wigner_into(rot_ref, vectors):
    x, y, z = vectors[0:1], vectors[1:2], vectors[2:3]
    length = jnp.sqrt(x * x + y * y + z * z)
    u = [x / length, y / length, z / length]
    pick = jnp.where(jnp.abs(u[0]) < 0.6, 1.0, 0.0)
    other = 1.0 - pick
    a = [-u[2] * other, u[2] * pick, u[0] * other - u[1] * pick]
    norm = jnp.sqrt(a[0] * a[0] + a[1] * a[1] + a[2] * a[2])
    a = [part / norm for part in a]
    b = [
        u[1] * a[2] - u[2] * a[1],
        u[2] * a[0] - u[0] * a[2],
        u[0] * a[1] - u[1] * a[0],
    ]
    shape = (8, x.shape[1])
    order = lax.broadcasted_iota(jnp.int32, shape, 0)
    wide = [jnp.broadcast_to(part, shape) for part in u]
    below = [jnp.where(order == 0, 1.0, 0.0)]
    rot_ref[0] = below[0]
    for l in range(1, LMAX + 1):
        table = RAISE[l]
        inverse = [1.0 / float(table[2][m + l, m + l - 1]) if m < l else 0.0 for m in range(3)]
        scale = jnp.where(
            order == 0, inverse[0], jnp.where(order <= 2, inverse[1], inverse[2])
        )
        rows = project(table, l, [part * scale for part in wide], below)
        rows = [jnp.zeros(shape, jnp.float32) if row is None else row for row in rows]
        if l == 1:
            first = project(table, 1, a, [1.0])
            second = project(table, 1, b, [1.0])
            one = 1.0 / float(table[0][2, 0])
            two = 1.0 / float(table[1][0, 0])
            rows = [
                jnp.where(order == 1, one * f, jnp.where(order == 2, two * s, r))
                for f, s, r in zip(first, second, rows)
            ]
        if l == 2:
            plus = [row[1:2] for row in below]
            minus = [row[2:3] for row in below]
            aa, bb = project(table, 2, a, plus), project(table, 2, b, minus)
            ab, ba = project(table, 2, a, minus), project(table, 2, b, plus)
            one = 1.0 / float(table[0][4, 2] - table[1][4, 0])
            two = 1.0 / float(table[0][0, 0] + table[1][0, 2])
            rows = [
                jnp.where(
                    order == 3,
                    one * (aa[m] - bb[m]),
                    jnp.where(order == 4, two * (ab[m] + ba[m]), rows[m]),
                )
                for m in range(5)
            ]
        for k, row in enumerate(rows):
            rot_ref[l * l + k] = row
        below = rows
    return length


STARTS = {"p1": 0, "n1": 768, "p2": 1536, "n2": 2176, "z": 2816}
LEFT_BLOCKS = 26


def left_rows(order, degree):
    if order == 0:
        return [(STARTS["z"] + 64 * degree, False)]
    m = (order + 1) // 2
    count = LMAX + 1 - m
    plus, minus = STARTS["p%d" % m], STARTS["n%d" % m]
    here = 64 * (degree - m)
    if order % 2:
        return [(plus + here, False), (minus + 64 * count + here, False)]
    return [(minus + here, False), (plus + 64 * count + here, True)]


def coefficient_row(k):
    return (k % TILES) * LANES + (k // TILES) * 64


GROUPS = [("z", (0, 1, 7)), ("y", (0,)), ("z", (2, 6)), ("y", (1, 3)), ("z", (3, 5, 4)), ("y", (2,))]


def group_tiles(axis):
    return range(0, Y_TILES) if axis == "z" else range(Y_TILES, TILES)


def group_needs(axis, offsets):
    return {
        (tile, oy, oz, side)
        for tile in group_tiles(axis)
        for oy in (range(Y_RING) if axis == "z" else offsets)
        for oz in (offsets if axis == "z" else range(Z_RING))
        for side in ("own", "other")
    }


PIECES = [
    ((6,), 36, 7, 6),
    ((5,), 25, 6, 5),
    ((4,), 16, 5, 4),
    ((3,), 9, 4, 3),
    ((0, 1, 2), 0, 5, 4),
]
PART_ROWS = 16 * sum(piece[2] for piece in PIECES)


def layer_kernel(
    nodes_hbm,
    vector_hbm,
    part_hbm,
    slot_hbm,
    target_hbm,
    live_ref,
    zero_hbm,
    one_hbm,
    two_hbm,
    out_ref,
    nodes_ref,
    vector_ref,
    part_ref,
    slot_ref,
    target_ref,
    table_ref,
    vectors_ref,
    zero_ref,
    one_ref,
    two_ref,
    rot_ref,
    pick_ref,
    states_ref,
    rows_ref,
    left_ref,
    mixed_ref,
    parts_ref,
    landing_ref,
    send,
    recv,
    local,
    spread_sems,
    part_sems,
):
    edge = lax.axis_index("edge")
    chan = lax.axis_index("chan")
    edges = part_ref.shape[1]
    reads = [
        pltpu.make_async_copy(src, dst, local.at[3 + index])
        for index, (src, dst) in enumerate(
            (
                (nodes_hbm, nodes_ref),
                (vector_hbm, vector_ref),
                (part_hbm, part_ref),
                (slot_hbm, slot_ref),
                (target_hbm, target_ref),
            )
        )
    ]
    for read in reads:
        read.start()
    x = edge % 2
    z = (edge // 2) % Z_RING
    y = edge // (2 * Z_RING)

    def wrap(position, offset, size):
        return (position + (offset % size)) % size

    def device(dy, dz, side):
        return (wrap(y, dy, Y_RING) * Z_RING + wrap(z, dz, Z_RING)) * 2 + side

    reach = {link: device(dy, dz, x) for link, (dy, dz) in STEP.items() if link != "x"}
    reach["x"] = device(0, 0, 1 - x)
    barrier = pltpu.get_barrier_semaphore()
    for target in reach.values():
        pl.semaphore_signal(
            barrier, inc=1, device_id={"edge": target, "chan": chan}, device_id_type=MESH
        )
    for far in range(1, 4):
        pl.semaphore_signal(
            barrier,
            inc=1,
            device_id={"edge": edge, "chan": (chan + far) % 4},
            device_id_type=MESH,
        )
    loads = [
        pltpu.make_async_copy(src, dst, local.at[index])
        for index, (src, dst) in enumerate(
            ((one_hbm, one_ref), (two_hbm, two_ref), (zero_hbm, zero_ref))
        )
    ]
    for read in reads:
        read.wait()
    for tile in range(TILES):
        low = nodes_ref[tile]
        high = nodes_ref[tile + TILES] if tile + TILES < COEFS else jnp.zeros_like(low)
        table_ref[y, z, x, tile] = jnp.concatenate([low, high], axis=1)
    vectors_ref[chan] = vector_ref[...]
    pl.semaphore_wait(barrier, 8)

    copies = []
    span = {"both": pl.ds(0, 2), "own": pl.ds(x, 1), "other": pl.ds(1 - x, 1)}
    for index, (link, sides, first, end, oy, oz) in enumerate(SENDS):
        view = table_ref.at[
            wrap(y, oy, Y_RING),
            wrap(z, oz, Z_RING),
            span[sides],
            pl.ds(first, end - first),
        ]
        copies.append(
            pltpu.make_async_remote_copy(
                src_ref=view,
                dst_ref=view,
                send_sem=send.at[index],
                recv_sem=recv.at[index],
                device_id={"edge": reach[link], "chan": chan},
                device_id_type=MESH,
            )
        )
    spread = [
        pltpu.make_async_remote_copy(
            src_ref=vector_ref,
            dst_ref=vectors_ref.at[chan],
            send_sem=spread_sems.at[far - 1],
            recv_sem=spread_sems.at[far + 2],
            device_id={"edge": edge, "chan": (chan + far) % 4},
            device_id_type=MESH,
        )
        for far in range(1, 4)
    ]

    scaling = []

    def begin_loads():
        for load in loads:
            load.start()

    def make_rotation():
        for copy in spread:
            copy.wait_recv()
        vectors = jnp.concatenate([vectors_ref[part] for part in range(4)], axis=1)
        length = wigner_into(rot_ref, vectors)
        alive = lax.broadcasted_iota(jnp.int32, (1, edges), 1) < live_ref[0]
        scaling.append(
            jnp.where(alive, 0.5 * (jnp.cos(length * (math.pi / CUTOFF)) + 1.0), 0.0)
        )

    def make_pick():
        source = part_ref[...] * 16 + slot_ref[...]
        row = lax.broadcasted_iota(jnp.int32, (32, edges), 0)
        for part in range(Y_RING * Z_RING):
            pick_ref[part // Z_RING, part % Z_RING] = jnp.where(
                source == row + 32 * part, 1.0, 0.0
            ).astype(jnp.bfloat16)

    def pick(axis, offsets, first, count, fresh):
        right, left = [], []
        for offset in offsets:
            if axis == "z":
                where = wrap(z, offset, Z_RING)
                right.append(pick_ref[:, where].reshape(128, edges))
            else:
                where = wrap(y, offset, Y_RING)
                right.append(pick_ref[where].reshape(256, edges))
            tiles = []
            for tile in range(first, first + count):
                if axis == "z":
                    part = table_ref[:, where, :, tile].reshape(128, LANES)
                else:
                    part = table_ref[where, :, :, tile].reshape(256, LANES)
                tiles.append(part.T)
            left.append(jnp.concatenate(tiles, axis=0) if count > 1 else tiles[0])
        left = jnp.concatenate(left, axis=1) if len(left) > 1 else left[0]
        right = jnp.concatenate(right, axis=0) if len(right) > 1 else right[0]
        picked = jnp.dot(left, right, preferred_element_type=jnp.float32).astype(jnp.bfloat16)
        rows = pl.ds(first * LANES, count * LANES)
        states_ref[rows, :] = picked if fresh else states_ref[rows, :] + picked

    have = {(tile, 0, 0, "own") for tile in range(TILES)}
    groups = list(GROUPS)
    seen = set()
    work = [begin_loads, make_pick, make_rotation]
    for kind, index in PROGRAM:
        if kind == "send":
            copies[index].start()
            if index == 3:
                for copy in spread:
                    copy.start()
            continue
        if index >= 10 and work:
            work.pop(0)()
        copies[index].wait_recv()
        have |= brought(index)
        while groups and group_needs(*groups[0]) <= have:
            axis, offsets = groups.pop(0)
            tiles = group_tiles(axis)
            for first in range(tiles[0], tiles[-1] + 1, 2):
                count = min(2, tiles[-1] + 1 - first)
                fresh = axis not in seen
                work.append(
                    lambda a=axis, o=offsets, f=first, c=count, n=fresh: pick(a, o, f, c, n)
                )
            seen.add(axis)
    for item in work:
        item()

    scale = jnp.broadcast_to(scaling[0], (16, edges))
    for degree in range(LMAX + 1):
        orders = 2 * min(degree, MMAX) + 1
        base = degree * degree

        def turn(chunk, carry, degree=degree, orders=orders, base=base):
            start = pl.multiple_of(chunk * 16, 16)
            totals = [None] * orders
            for k in range(2 * degree + 1):
                rows = pl.ds(coefficient_row(base + k) + start, 16)
                value = states_ref[rows, :].astype(jnp.float32)
                for order in range(orders):
                    factor = rot_ref[base + k, order : order + 1, :]
                    term = factor * value
                    totals[order] = term if k == 0 else totals[order] + term
            for order in range(orders):
                result = totals[order] * scale
                for first, negate in left_rows(order, degree):
                    rows_ref[pl.ds(first + start, 16), :] = (
                        -result if negate else result
                    ).astype(jnp.bfloat16)
            return carry

        lax.fori_loop(0, 4, turn, 0)

    def flip(block, carry):
        rows = pl.ds(pl.multiple_of(block * LANES, LANES), LANES)
        left_ref[block] = rows_ref[rows, :].T
        return carry

    lax.fori_loop(0, LEFT_BLOCKS, flip, 0)
    slot = lax.broadcasted_iota(jnp.int32, (16, edges), 0)
    chosen = jnp.where(slot == target_ref[...], 1.0, 0.0)

    def left(first, depth):
        blocks = [left_ref[first // LANES + i] for i in range(-(-depth // LANES))]
        return jnp.concatenate(blocks, axis=1)[:, :depth]

    def mix(turn_of, order, start, depth, right):
        mixed = jnp.dot(left(start, depth), right, preferred_element_type=jnp.float32)
        mixed_ref[turn_of, order] = mixed.astype(jnp.bfloat16)

    def degree_sum(degree, turn_of):
        mix(turn_of, 0, STARTS["z"], 448, zero_ref[:, degree].reshape(448, 256))
        if degree >= 1:
            right = one_ref[:, :, degree - 1].reshape(768, 256)
            mix(turn_of, 1, STARTS["p1"], 768, right)
            mix(turn_of, 2, STARTS["n1"], 768, right)
        if degree >= 2:
            right = two_ref[:, :, degree - 2].reshape(640, 256)
            mix(turn_of, 3, STARTS["p2"], 640, right)
            mix(turn_of, 4, STARTS["n2"], 640, right)
        orders = 2 * min(degree, MMAX) + 1
        back = [
            jnp.concatenate(
                [
                    (rot_ref[degree * degree + k, order : order + 1, :] * chosen).astype(
                        jnp.bfloat16
                    )
                    for k in range(2 * degree + 1)
                ],
                axis=0,
            )
            for order in range(orders)
        ]
        back = jnp.concatenate(back, axis=1) if orders > 1 else back[0]
        mixed = mixed_ref[turn_of, 0:orders].reshape(orders * edges, 256)
        return jnp.dot(back, mixed, preferred_element_type=jnp.float32)

    for load in loads:
        load.wait()
    outgoing = []
    base = 0
    for number, (degrees, first, lows, highs) in enumerate(PIECES):
        sums = [degree_sum(degree, degree % 2) for degree in degrees]
        sums = jnp.concatenate(sums, axis=0) if len(sums) > 1 else sums[0]
        if highs < lows:
            sums = jnp.concatenate([sums, jnp.zeros((16, 256), jnp.float32)], axis=0)
        for part in range(4):
            lanes = slice(64 * part, 64 * part + 64)
            parts_ref[part, pl.ds(16 * base, 16 * lows)] = jnp.concatenate(
                [sums[: 16 * lows, lanes], sums[16 * lows :, lanes]], axis=1
            ).astype(jnp.bfloat16)
        piece = []
        for far in (2, 1, 3):
            target = (chan + far) % 4
            copy = pltpu.make_async_remote_copy(
                src_ref=parts_ref.at[target, pl.ds(16 * base, 16 * lows)],
                dst_ref=landing_ref.at[far - 1, pl.ds(16 * base, 16 * lows)],
                send_sem=part_sems.at[0, number, far - 1],
                recv_sem=part_sems.at[1, number, far - 1],
                device_id={"edge": edge, "chan": target},
                device_id_type=MESH,
            )
            copy.start()
            piece.append(copy)
        outgoing.append((base, piece))
        base += lows
    for copy in copies + spread:
        copy.wait_send()
    for (base, piece), (degrees, first, lows, highs) in zip(outgoing, PIECES):
        for copy in piece:
            copy.wait_recv()
        rows = pl.ds(16 * base, 16 * lows)
        total = parts_ref[chan, rows].astype(jnp.float32)
        for slot_number in range(3):
            total = total + landing_ref[slot_number, rows].astype(jnp.float32)
        total = total.astype(jnp.bfloat16)
        for step in range(lows):
            out_ref[first + step] = total[16 * step : 16 * step + 16, :64]
        for step in range(highs):
            out_ref[first + lows + step] = total[16 * step : 16 * step + 16, 64:]
    for _, piece in outgoing:
        for copy in piece:
            copy.wait_send()


def shards(
    node_states,
    edge_vectors,
    source_part,
    source_slot,
    target_slot,
    live_edges,
    weight_zero,
    weight_one,
    weight_two,
):
    edges = source_slot.shape[0]
    zero = weight_zero.transpose(0, 2, 1, 3)
    one = weight_one.transpose(0, 1, 3, 2, 4)
    two = weight_two.transpose(0, 1, 3, 2, 4)
    vmem = pl.BlockSpec(memory_space=pltpu.VMEM)
    hbm = pl.BlockSpec(memory_space=pl.ANY)
    result = pl.pallas_call(
        layer_kernel,
        name="layer",
        out_shape=jax.ShapeDtypeStruct((COEFS, 16, 64), jnp.bfloat16),
        in_specs=[hbm] * 5 + [pl.BlockSpec(memory_space=pltpu.SMEM), hbm, hbm, hbm],
        out_specs=vmem,
        scratch_shapes=[
            pltpu.VMEM((COEFS, 16, 64), jnp.bfloat16),
            pltpu.VMEM((3, LANES), jnp.float32),
            pltpu.VMEM((1, edges), jnp.int32),
            pltpu.VMEM((1, edges), jnp.int32),
            pltpu.VMEM((1, edges), jnp.int32),
            pltpu.VMEM((Y_RING, Z_RING, 2, TILES, 16, LANES), jnp.bfloat16),
            pltpu.VMEM((4, 3, LANES), jnp.float32),
            pltpu.VMEM(zero.shape, jnp.bfloat16),
            pltpu.VMEM(one.shape, jnp.bfloat16),
            pltpu.VMEM(two.shape, jnp.bfloat16),
            pltpu.VMEM((COEFS, 8, edges), jnp.float32),
            pltpu.VMEM((Y_RING, Z_RING, 32, edges), jnp.bfloat16),
            pltpu.VMEM((TILES * LANES, edges), jnp.bfloat16),
            pltpu.VMEM((LEFT_BLOCKS * LANES, edges), jnp.bfloat16),
            pltpu.VMEM((LEFT_BLOCKS, edges, LANES), jnp.bfloat16),
            pltpu.VMEM((2, 5, edges, 256), jnp.bfloat16),
            pltpu.VMEM((4, PART_ROWS, LANES), jnp.bfloat16),
            pltpu.VMEM((3, PART_ROWS, LANES), jnp.bfloat16),
            pltpu.SemaphoreType.DMA((len(SENDS),)),
            pltpu.SemaphoreType.DMA((len(SENDS),)),
            pltpu.SemaphoreType.DMA((8,)),
            pltpu.SemaphoreType.DMA((6,)),
            pltpu.SemaphoreType.DMA((2, len(PIECES), 3)),
        ],
        compiler_params=pltpu.CompilerParams(
            collective_id=0, has_side_effects=True, vmem_limit_bytes=60 << 20
        ),
    )(
        node_states.transpose(1, 0, 2),
        edge_vectors,
        source_part.reshape(1, edges),
        source_slot.reshape(1, edges),
        target_slot.reshape(1, edges),
        live_edges,
        zero,
        one,
        two,
    )
    return result.transpose(1, 0, 2)


def solution(mesh):
    in_specs = (
        P("edge", None, "chan"),
        P(None, ("edge", "chan")),
        P("edge", None),
        P("edge"),
        P("edge"),
        P("edge"),
        P(None, "chan", None, None),
        P(None, None, "chan", None, None),
        P(None, None, "chan", None, None),
    )
    out_specs = P("edge", None, "chan")
    return jax.shard_map(shards, mesh=mesh, in_specs=in_specs, out_specs=out_specs, check_vma=False)
```
